32 devices in a mesh: mkt: 8 (over z, x), grp: 4 (over y, core).
Axes of the slice: x: 2, y: 2, z: 4, core: 2. Of those that a mesh axis runs over, the one named last changes fastest.
Arguments:
- mean_utility: float32 [512, 64], P(('mkt', 'grp')), may hold values from -5 to -1
- market_share: float32 [512, 64], P(('mkt', 'grp')), may hold values from 0.001 to 0.02
- product_traits: float32 [512, 64, 5], P(('mkt', 'grp')), may hold values from -1 to 1
- taste_draws: float32 [512, 5, 1024], P(('mkt', 'grp')), may hold values from -4 to 4
- taste_scale: float32 [5], replicated, may hold values from 0.3 to 1
- type_weight: float32 [512, 1024], P(('mkt', 'grp')), may hold values from 0.1 to 1
- market_size: float32 [512], P(('mkt', 'grp')), may hold values from 0.05 to 3
- product_firm: int32 [512, 64], P(('mkt', 'grp')), may hold values from 0 to 511, all different within a row
- firm_order: int32 [512], replicated, may hold values from 0 to 511, each once
- loyalty: float32 [512, 1024], P(('mkt', 'grp')), may hold values from -1 to 1
- firm_share: float32 [512, 1024], replicated, may hold values from 2e-05 to 0.15
Outputs:
- utility_out: float32 [512, 64], P(('mkt', 'grp'))
- loyalty_out: float32 [512, 1024], P(('mkt', 'grp'))
The draws below stay inside these ranges and needn't reach their ends.
Inputs may be any that keep to these rules, and one draw needn't show every extreme that they name: `product_firm`: in each market the 64 products belong to 64 different firms, and every firm sells in some market. `firm_order`: each firm appears once.
All inputs are finite; a program needn't handle non-finite values.
Results may differ from the reference program's by a relative error of at most 0.0001.
Values sent between devices are 32-bit elements; how exact they have to be, the bound alone decides.
A program may use at most 64 MiB of HBM per device.

```python
import math
import jax
import jax.numpy as jnp
from jax import lax

J = 64
FIRMS = 512
R = 1024
K = 5
ITERS = 3
M_DEV = 16
MARKETS = 512


def draw_market_size(key, part):
    index = jnp.arange(MARKETS, dtype=jnp.float32)
    base = 1.0 + 2.0 * index / max(MARKETS - 1, 1)
    factor = jnp.exp(jax.random.uniform(key, (MARKETS,), jnp.float32, jnp.log(0.05), 0.0))
    return base * factor


def draw_firm_share(key, part):
    key_firm = jax.random.fold_in(key, 11)
    key_type = jax.random.fold_in(key, 12)
    key_noise = jax.random.fold_in(key, 13)
    firm_level = jax.random.uniform(key_firm, (FIRMS, 1), jnp.float32, -2.5, 2.5)
    noise = jnp.clip(0.5 * jax.random.normal(key_noise, (FIRMS, R), jnp.float32), -1.0, 1.0)
    type_level = jax.random.uniform(key_type, (1, R), jnp.float32, -0.5, 0.5)
    return jnp.exp(-6.5 + firm_level + type_level + noise)


def shard_levels(stream_key, shape, cuts, low, high):
    level = 1.0
    for position, shards_of in cuts:
        draws = jax.random.uniform(jax.random.fold_in(jax.random.fold_in(stream_key, 6), position), (shards_of,), jnp.float32, low / len(cuts), high / len(cuts))
        level = level * jnp.repeat(jnp.exp(draws), shape[position] // shards_of).reshape((-1,) + (1,) * (len(shape) - 1 - position))
    return level


def distinct(own_key, rows, number_of, top, lift):
    ranking = jax.random.permutation(jax.random.fold_in(own_key, 1), number_of)
    pull = ranking
    for power in range(3):
        pull = pull * pull // number_of
    pull = pull * lift // number_of
    tickets = jax.random.randint(jax.random.fold_in(own_key, 2), (rows, number_of), 0, 4096) + pull
    fixed_rows = jax.random.permutation(jax.random.fold_in(own_key, 3), rows)[jnp.arange(number_of) % rows]
    tickets = jnp.where(jnp.arange(rows)[:, None] == fixed_rows[None, :], 1 << 14, tickets)
    score = tickets * number_of + jnp.arange(number_of)
    return lax.top_k(score.astype(jnp.int32), top)[1].astype(jnp.int32)


def scatter_about(stream_key, shape, spread, most, split=(), kind=jnp.bfloat16):
    level = shard_levels(stream_key, shape, split, -0.22, 0.18) if split else 1.0
    values = jax.random.normal(stream_key, shape, jnp.float32) * spread * level
    return jnp.minimum(jnp.maximum(values, -most), most).astype(kind)


def setup_inputs(seed: int = 0) -> dict:
    seeds = jax.random.split(jax.random.key(seed), 12)
    return {
        "mean_utility": jnp.clip(-5.0 + 4.0 * jax.random.uniform(seeds[0], (MARKETS, J), jnp.float32) ** shard_levels(seeds[0], (MARKETS, J), ((0, 32),), -0.2, 0.2), -5.0, -1.0),
        "market_share": jnp.clip(jnp.exp(math.log(0.02) - 2.9957322 * jax.random.uniform(seeds[1], (MARKETS, J), jnp.float32) ** shard_levels(seeds[1], (MARKETS, J), ((0, 32),), -0.2, 0.2)), 0.001, 0.02),
        "product_traits": jnp.clip(jax.random.uniform(seeds[2], (MARKETS, J, K), jnp.float32, -1.0, 1.0) * shard_levels(seeds[2], (MARKETS, J, K), ((0, 32),), -0.4, 0.0), -1.0, 1.0),
        "taste_draws": scatter_about(seeds[3], (MARKETS, K, R), 1.0, 4.0, ((0, 32),), jnp.float32),
        "taste_scale": jnp.clip(jnp.exp(jax.random.uniform(seeds[4], (K,), jnp.float32, math.log(0.3), math.log(1.0))), 0.3, 1.0),
        "type_weight": jnp.clip(jnp.exp(math.log(1.0) - 2.3025851 * jax.random.uniform(seeds[5], (MARKETS, R), jnp.float32) ** shard_levels(seeds[5], (MARKETS, R), ((0, 32),), -0.2, 0.2)), 0.1, 1.0),
        "market_size": draw_market_size(jax.random.fold_in(seeds[11], 71), 0),
        "product_firm": distinct(seeds[7], MARKETS, FIRMS, J, 1024),
        "firm_order": jax.random.permutation(seeds[8], FIRMS).astype(jnp.int32),
        "loyalty": jnp.clip(jax.random.uniform(seeds[9], (FIRMS, R), jnp.float32, -1.0, 1.0) * shard_levels(seeds[9], (FIRMS, R), ((0, 32),), -0.4, 0.0), -1.0, 1.0),
        "firm_share": draw_firm_share(jax.random.fold_in(seeds[11], 71), 0),
    }


clip_target = 0.5
norm_eps = 1e-06

def market_terms(mean_block, traits_block, draws_block, weight_block, size_block, firms_block, table, taste_scale):
    taste = jnp.einsum('mjk,mkr->mjr', traits_block * taste_scale, draws_block, precision=lax.Precision.HIGHEST)
    expu = jnp.exp(mean_block[:, :, None] + taste + jnp.take(table, firms_block, axis=0))
    choice_prob = expu / (1.0 + lax.optimization_barrier(jnp.sum(expu, axis=1, keepdims=True)))
    predicted = jnp.einsum('mjr,mr->mj', choice_prob, weight_block, precision=lax.Precision.HIGHEST) / lax.optimization_barrier(jnp.sum(weight_block, axis=1))[:, None]
    weighted = choice_prob * (size_block[:, None] * weight_block)[:, None, :]
    partial_value = jax.ops.segment_sum(weighted.reshape(-1, weighted.shape[2]), firms_block.reshape(-1), num_segments=table.shape[0])
    return (predicted, partial_value)

def reference(mean_utility, market_share, product_traits, taste_draws, taste_scale, type_weight, market_size, product_firm, firm_order, loyalty, firm_share):
    blocks = MARKETS // M_DEV
    table = jnp.zeros((FIRMS, R), loyalty.dtype).at[firm_order].set(loyalty)
    type_mass = lax.optimization_barrier(jnp.sum(market_size[:, None] * type_weight, axis=0))
    traits_b = product_traits.reshape(blocks, M_DEV, J, K)
    draws_b = taste_draws.reshape(blocks, M_DEV, K, R)
    weight_b = type_weight.reshape(blocks, M_DEV, R)
    size_b = market_size.reshape(blocks, M_DEV)
    firms_b = product_firm.reshape(blocks, M_DEV, J)
    mean_now = mean_utility
    for step in range(ITERS):
        mean_b = mean_now.reshape(blocks, M_DEV, J)

        def scan_block(carry, pieces):
            predicted, partial_value = market_terms(pieces[0], pieces[1], pieces[2], pieces[3], pieces[4], pieces[5], table, taste_scale)
            return (carry + partial_value, predicted)
        totals, predicted = lax.scan(scan_block, jnp.zeros((FIRMS, R), jnp.float32), (mean_b, traits_b, draws_b, weight_b, size_b, firms_b))
        gap = jnp.log(firm_share) - jnp.log(totals / type_mass[None, :])
        clip = jnp.minimum(1.0, clip_target / jnp.sqrt(jnp.mean(gap * gap) + norm_eps))
        table = table + clip * gap
        mean_now = mean_now + jnp.log(market_share) - jnp.log(predicted.reshape(MARKETS, J))
    return (mean_now, jnp.take(table, firm_order, axis=0))
```

```python
import functools

import jax
import jax.numpy as jnp
from jax import lax
from jax.experimental import pallas as pl
from jax.experimental.pallas import tpu as pltpu
from jax.sharding import PartitionSpec as P

ITERS = 3
LANES = 128
MESH = pl.DeviceIdType.MESH

clip_target = 0.5
norm_eps = 1e-06

scope = jax.named_scope


def columns(row):
    return jnp.broadcast_to(row, (LANES, LANES)).T


def split_hi_lo(x):
    hi = x.astype(jnp.bfloat16)
    lo = (x - hi.astype(jnp.float32)).astype(jnp.bfloat16)
    return hi, lo


def xor(x, d, size):
    out = x
    bit = 1
    while bit < size:
        out = out + ((d // bit) % 2) * (1 - 2 * ((x // bit) % 2)) * bit
        bit *= 2
    return out


def kernel(
    dims,
    size_h, scale_h, draws_h, weight_h, traits_h, firm_h, mean_h, share_own_h, loy_h, order_h, share_h,
    mean_out, loy_out,
    size_ref, scale_ref, weight_ref, traits_ref, firm_ref, mean_ref, share_own_ref, order_ref, share_v,
    draws, mass, info, loy, means, tbl, tq, tmass, tm_own,
    mass_own, lmat, rmat, one_hot, util, near_gap, col, order_col, order_row, table_hl, weighted,
    sums, sums_in, totals, totals_in, gap, squares, squares_in, old, old_in, last, last_in,
    in_s, draws_s, mass_s, info_s, loy_s, mean_s, tq_s, tm_s, sums_s, totals_s, gap_s, old_s, last_s, sq_s,
):
    mkt, grp, rb, groups, n_m, J, K, firms, owned, R = dims
    n = mkt * grp
    rows = n_m * J
    tiles = rows // LANES
    pair = LANES // J
    qr = firms // groups
    half = groups // 2
    near = half * qr
    a = lax.axis_index("mkt")
    b = lax.axis_index("grp")
    ao, ai = a // rb, a % rb
    q_me = ao * grp + b
    me = a * grp + b

    def type_lane(d):
        return xor(ai, d, rb)

    def type_device(d):
        return (ao * rb + xor(ai, d, rb), b)

    def market_device(j):
        q = xor(q_me, j, groups)
        return ((q // grp) * rb + ai, q % grp)

    def lanes_of(p):
        return pl.ds(pl.multiple_of(p * LANES, LANES), LANES)

    pending = []

    def send(src, dst, sems, slot, device):
        copy = pltpu.make_async_remote_copy(
            src_ref=src, dst_ref=dst, send_sem=sems.at[0, slot], recv_sem=sems.at[1, slot],
            device_id=device, device_id_type=MESH,
        )
        copy.start()
        pending.append(copy)

    def arrive(dst, sems, slot):
        pltpu.make_async_copy(dst, dst, sems.at[1, slot]).wait()

    def pack(x):
        return jnp.concatenate([x[i * tiles:(i + 1) * tiles, :] for i in range(pair)], axis=1)

    inputs = {}
    for at, (key, src, dst) in enumerate((
        ("weight", weight_h, weight_ref), ("traits", traits_h, traits_ref), ("firm", firm_h, firm_ref),
        ("mean", mean_h, mean_ref), ("size", size_h, size_ref), ("scale", scale_h, scale_ref),
        ("draws", draws_h.at[:, lanes_of(ai)], draws.at[0]), ("loy", loy_h.at[:, lanes_of(ai)], loy.at[0]),
        ("order", order_h, order_ref), ("share_own", share_own_h, share_own_ref),
        ("share", share_h.at[:, lanes_of(ai)], share_v),
    )):
        inputs[key] = pltpu.make_async_copy(src, dst, in_s.at[at])
        inputs[key].start()

    barrier = pltpu.get_barrier_semaphore()

    @pl.loop(1, n)
    def _(d):
        t = (me + d) % n
        pl.semaphore_signal(barrier, inc=1, device_id=(t // grp, t % grp), device_id_type=MESH)

    for key in ("weight", "traits", "firm", "mean", "size", "scale"):
        inputs[key].wait()
    for k in range(K):
        info[0, k] = pack(traits_ref[k] * scale_ref[k])
    info[0, K] = pack(firm_ref[...].astype(jnp.float32))
    mean_now = pack(mean_ref[...])
    info[0, K + 1] = mean_now
    for m in range(n_m):
        mass_own[m:m + 1, :] = weight_ref[m:m + 1, :] * size_ref[m]

    with scope("bar"):
        pl.semaphore_wait(barrier, n - 1)

    for d in range(1, rb):
        send(loy_h.at[:, lanes_of(type_lane(d))], loy.at[d], loy_s, d, type_device(d))
    for d in range(1, rb):
        device = type_device(d)
        lanes = lanes_of(type_lane(d))
        send(draws_h.at[:, lanes], draws.at[d], draws_s, d, device)
        send(info.at[0], info.at[d], info_s, d, device)
        send(mass_own.at[:, lanes], mass.at[d], mass_s, d, device)

    mass[0] = mass_own[:, lanes_of(ai)]

    for key in ("order", "draws", "loy"):
        inputs[key].wait()
    for i in range(firms // LANES):
        col[i * LANES:(i + 1) * LANES, :] = columns(order_ref[i:i + 1, :].astype(jnp.float32))
    for j in range(groups):
        q = xor(q_me, j, groups)
        for d in range(rb):
            src = (((q // grp) * rb + xor(ai, d, rb)) * grp + q % grp) * owned
            dst = (j * rb + d) * owned
            order_col[dst:dst + owned, :] = col[pl.ds(pl.multiple_of(src, owned), owned), :]
    for i in range(firms // LANES):
        order_row[0:1, i * LANES:(i + 1) * LANES] = order_col[i * LANES:(i + 1) * LANES, :].T[0:1, :]

    kk = n_m * K
    row = lax.broadcasted_iota(jnp.int32, (n_m, LANES), 0)
    lane = lax.broadcasted_iota(jnp.int32, (n_m, LANES), 1)
    offset = row - (lane // J) * tiles
    zero = jnp.zeros((n_m, LANES), jnp.float32)
    rmat[kk:, :] = jnp.zeros_like(rmat[kk:, :])
    rmat[2 * kk:, :LANES] = jnp.ones_like(rmat[2 * kk:, :LANES])

    def rows_of(d, r0, count):
        return pl.ds(pl.multiple_of(d * rows + r0, LANES), count)

    def spread(part, where):
        return jnp.where(where, jnp.broadcast_to(part.astype(jnp.float32), (n_m, LANES)), zero).astype(jnp.bfloat16)

    def prepare(d):
        hi, lo = split_hi_lo(draws[d])
        rmat[:kk, :LANES] = hi
        rmat[:kk, LANES:] = lo
        rmat[kk:2 * kk, :LANES] = hi
        for i in range(tiles):
            here = offset == i
            at = slice(i * LANES, (i + 1) * LANES)
            for k in range(K):
                hi, lo = split_hi_lo(info[d, k, i:i + 1, :])
                lmat[k * n_m:(k + 1) * n_m, at] = spread(hi, here)
                lmat[kk + k * n_m:kk + (k + 1) * n_m, at] = spread(lo, here)
            rest = info[d, K + 1, i:i + 1, :]
            for s in range(3):
                hi = rest.astype(jnp.bfloat16)
                rest = rest - hi.astype(jnp.float32)
                lmat[2 * kk + s * n_m:2 * kk + (s + 1) * n_m, at] = spread(hi, here)
        both = lax.dot_general(
            lmat[...], rmat[...], (((0,), (0,)), ((), ())), preferred_element_type=jnp.float32
        )
        util[rows_of(d, 0, rows), :] = both[:, :LANES] + both[:, LANES:]
        for i in range(tiles):
            firm_col = columns(info[d, K, i:i + 1, :])
            for f in range(firms // LANES):
                one_hot[rows_of(d, i * LANES, LANES), f * LANES:(f + 1) * LANES] = (
                    firm_col == order_row[0:1, f * LANES:(f + 1) * LANES]
                ).astype(jnp.float32).astype(jnp.bfloat16)

    with scope("prep0"):
        prepare(0)

    with scope("arr_loy"):
        for d in range(1, rb):
            arrive(loy.at[d], loy_s, d)
    for d in range(rb):
        tq[d * owned:(d + 1) * owned, :] = loy[d]
    for j in range(1, groups):
        send(tq, tbl.at[j], tq_s, j, market_device(j))
    tbl[0] = tq[...]

    def arrive_inputs(d):
        arrive(info.at[d], info_s, d)
        arrive(draws.at[d], draws_s, d)
        arrive(mass.at[d], mass_s, d)

    first = rb // 2

    @pl.loop(1, first)
    def _(d):
        with scope("arr_a"):
            arrive_inputs(d)
        with scope("prep_a"):
            prepare(d)

    with scope("share"):
        inputs["share"].wait()
        inputs["share_own"].wait()
        mine_col = order_col[:qr, :]
        number = lax.broadcasted_iota(jnp.int32, (qr, LANES), 1).astype(jnp.float32)
        my_share = jnp.zeros((qr, LANES), jnp.float32)
        for i in range(firms // LANES):
            pick = (mine_col == number + float(i * LANES)).astype(jnp.float32)
            my_share += jnp.dot(
                pick, share_v[i * LANES:(i + 1) * LANES, :],
                precision=lax.Precision.HIGHEST, preferred_element_type=jnp.float32,
            )
        my_share = jnp.log(my_share)
        base = jnp.log(share_own_ref[...]) + jnp.log(jnp.sum(mass_own[...], axis=1, keepdims=True))
        base = pack(base)

    with scope("arr_tbl"):
        for j in range(1, groups):
            arrive(tbl.at[j], tq_s, j)

    def split_into(j, value):
        hi, lo = split_hi_lo(value)
        table_hl[j * qr:(j + 1) * qr, :LANES] = hi
        table_hl[j * qr:(j + 1) * qr, LANES:] = lo

    for j in range(groups):
        split_into(j, tbl[j])

    per_block = 2
    block = per_block * LANES

    def gather(d, r0, begin, end):
        both = jnp.dot(
            one_hot[rows_of(d, r0, block), begin:end], table_hl[begin:end, :], preferred_element_type=jnp.float32
        )
        return both[:, :LANES] + both[:, LANES:]

    def shares(it, d, clip):
        for h in range(rows // block):
            r0 = h * block
            at = rows_of(d, r0, block)
            if it == 0:
                u = util[at, :] + gather(d, r0, 0, firms)
            else:
                u = util[at, :] + clip * (near_gap[at, :] + gather(d, r0, near, firms))
            if it < ITERS - 1:
                util[at, :] = u
            expu = jnp.exp(u)
            for i in range(per_block):
                t = h * per_block + i
                parts = []
                for s in range(pair):
                    part = expu[i * LANES + s * J:i * LANES + (s + 1) * J, :]
                    m = s * tiles + t
                    parts.append(
                        part * (mass[d, m:m + 1, :] / (1.0 + jnp.sum(part, axis=0, keepdims=True)))
                    )
                bought = jnp.concatenate(parts, axis=0).T
                sums[it, d, t:t + 1, :] = jnp.sum(bought, axis=0, keepdims=True)
                hi, lo = split_hi_lo(bought)
                lanes = rows_of(d, t * LANES, LANES)
                weighted[:LANES, lanes] = hi
                weighted[LANES:, lanes] = lo

    def half_totals(it, begin):
        acc = jnp.dot(
            weighted[...], one_hot[:, begin * qr:(begin + half) * qr], preferred_element_type=jnp.float32
        )
        acc = acc[:LANES, :] + acc[LANES:, :]
        acc = jnp.concatenate([acc[:, i * LANES:(i + 1) * LANES].T for i in range(near // LANES)], axis=0)
        for j in range(half):
            totals[it, begin + j] = acc[j * qr:(j + 1) * qr, :]

    clip = None
    log_mass = None
    for it in range(ITERS):
        final = it == ITERS - 1
        if it == 0:
            with scope("sh_a"):
                @pl.loop(0, first)
                def _(d):
                    shares(0, d, None)

            @pl.loop(first, rb)
            def _(d):
                with scope("arr_b"):
                    arrive_inputs(d)
                with scope("prep_b"):
                    prepare(d)
                with scope("sh_b"):
                    shares(0, d, None)

            tm_own[...] = jnp.zeros_like(tm_own)
            for d in range(rb):
                tm_own[...] += jnp.sum(mass[d], axis=0, keepdims=True)
            for j in range(1, groups):
                send(tm_own, tmass.at[j], tm_s, j, market_device(j))
            tmass[0] = tm_own[...]
        else:
            with scope("shares%d" % it):
                @pl.loop(0, rb)
                def _(d):
                    shares(it, d, clip)

        for d in range(1, rb):
            send(sums.at[it, d], sums_in.at[it, d], sums_s.at[it], d, type_device(d))
        sums_in[it, 0] = sums[it, 0]

        with scope("far%d" % it):
            half_totals(it, half)
        for j in range(half, groups):
            send(totals.at[it, j], totals_in.at[it, j], totals_s.at[it], j, market_device(j))
        with scope("near%d" % it):
            half_totals(it, 0)
        for j in range(1, half):
            send(totals.at[it, j], totals_in.at[it, j], totals_s.at[it], j, market_device(j))
        totals_in[it, 0] = totals[it, 0]

        if final:
            for d in range(rb):
                old[d] = tbl[0, d * owned:(d + 1) * owned, :]
            for d in range(1, rb):
                send(old.at[d], old_in.at[d], old_s, d, type_device(d))
            old_in[0] = old[0]

        if it == 0:
            for j in range(1, groups):
                arrive(tmass.at[j], tm_s, j)
            log_mass = jnp.log(jnp.sum(tmass[...], axis=0))

        with scope("arr_sums%d" % it):
            for d in range(1, rb):
                arrive(sums_in.at[it, d], sums_s.at[it], d)
        step = base - jnp.log(jnp.sum(sums_in[it], axis=0))
        mean_now = mean_now + step
        if final:
            for i in range(pair):
                mean_out[i * tiles:(i + 1) * tiles, :] = mean_now[:, i * J:(i + 1) * J]
        else:
            means[it, 0] = step
            for d in range(1, rb):
                send(means.at[it, 0], means.at[it, d], mean_s.at[it], d, type_device(d))

        with scope("arr_tot%d" % it):
            for j in range(1, groups):
                arrive(totals_in.at[it, j], totals_s.at[it], j)
        gap_mine = my_share - (jnp.log(jnp.sum(totals_in[it], axis=0)) - log_mass)
        squares[it] = jnp.sum(gap_mine * gap_mine, axis=0, keepdims=True)

        @pl.loop(1, n)
        def _(d):
            t = (me + d) % n
            pltpu.make_async_remote_copy(
                src_ref=squares.at[it], dst_ref=squares_in.at[it, d - 1],
                send_sem=sq_s.at[0, it], recv_sem=sq_s.at[1, it],
                device_id=(t // grp, t % grp), device_id_type=MESH,
            ).start()

        if final:
            for d in range(rb):
                last[d] = gap_mine[d * owned:(d + 1) * owned, :]
            for d in range(1, rb):
                send(last.at[d], last_in.at[d], last_s, d, type_device(d))
            last_in[0] = last[0]
        else:
            gap[it, 0] = gap_mine
            for j in [*range(half, groups), *range(1, half)]:
                send(gap.at[it, 0], gap.at[it, j], gap_s.at[it], j, market_device(j))
            for j in range(half):
                if j:
                    arrive(gap.at[it, j], gap_s.at[it], j)
                split_into(j, gap[it, j])

            with scope("gnear%d" % it):
                @pl.loop(0, rb)
                def _(d):
                    for r0 in range(0, rows, block):
                        near_gap[rows_of(d, r0, block), :] = gather(d, r0, 0, near)

            with scope("arr_mean%d" % it):
                for d in range(1, rb):
                    arrive(means.at[it, d], mean_s.at[it], d)

            with scope("addmean%d" % it):
                @pl.loop(0, rb)
                def _(d):
                    for i in range(tiles):
                        at = rows_of(d, i * LANES, LANES)
                        util[at, :] = util[at, :] + columns(means[it, d, i:i + 1, :])

            with scope("arr_gap%d" % it):
                for j in range(half, groups):
                    arrive(gap.at[it, j], gap_s.at[it], j)
                    split_into(j, gap[it, j])

        with scope("arr_sq%d" % it):
            pltpu.make_async_copy(squares_in.at[it], squares_in.at[it], sq_s.at[1, it]).wait()
        total = jnp.sum(jnp.sum(squares_in[it], axis=0) + squares[it], axis=1, keepdims=True)
        clip = jnp.minimum(1.0, clip_target / jnp.sqrt(total / (firms * R) + norm_eps))

        if final:
            with scope("arr_last"):
                for d in range(1, rb):
                    arrive(old_in.at[d], old_s, d)
                    arrive(last_in.at[d], last_s, d)
            for d in range(rb):
                loy_out[:, lanes_of(type_lane(d))] = old_in[d] + clip * last_in[d]
        else:
            tbl[0] = tbl[0] + clip * gap_mine

    with scope("drain"):
        for it in range(ITERS):
            pltpu.make_async_copy(squares_in.at[it], squares_in.at[it], sq_s.at[0, it]).wait()
        for copy in pending:
            copy.wait_send()


def local(
    mkt, grp,
    mean_utility, market_share, product_traits, taste_draws, taste_scale, type_weight,
    market_size, product_firm, firm_order, loyalty, firm_share,
):
    n_m, J, K = product_traits.shape
    firms, R = firm_share.shape
    owned = loyalty.shape[0]
    rb = R // LANES
    groups = mkt * grp // rb
    rows = n_m * J
    tiles = rows // LANES
    qr = firms // groups
    depth = n_m * (2 * K + 3)

    f32, bf16 = jnp.float32, jnp.bfloat16
    dma = pltpu.SemaphoreType.DMA
    vmem = pltpu.VMEM
    spec = pl.BlockSpec(memory_space=pltpu.VMEM)
    dims = (mkt, grp, rb, groups, n_m, J, K, firms, owned, R)
    scratch = [
        pltpu.SMEM((n_m,), f32),
        pltpu.SMEM((K,), f32),
        vmem((n_m, R), f32),
        vmem((K, n_m, J), f32),
        vmem((n_m, J), jnp.int32),
        vmem((n_m, J), f32),
        vmem((n_m, J), f32),
        vmem((firms // LANES, LANES), jnp.int32),
        vmem((firms, LANES), f32),
        vmem((rb, n_m * K, LANES), f32),
        vmem((rb, n_m, LANES), f32),
        vmem((rb, K + 2, tiles, LANES), f32),
        vmem((rb, owned, LANES), f32),
        vmem((ITERS - 1, rb, tiles, LANES), f32),
        vmem((groups, qr, LANES), f32),
        vmem((qr, LANES), f32),
        vmem((groups, 1, LANES), f32),
        vmem((1, LANES), f32),
        vmem((n_m, R), f32),
        vmem((depth, rows), bf16),
        vmem((depth, 2 * LANES), bf16),
        vmem((rb * rows, firms), bf16),
        vmem((rb * rows, LANES), f32),
        vmem((rb * rows, LANES), f32),
        vmem((firms, LANES), f32),
        vmem((firms, LANES), f32),
        vmem((1, firms), f32),
        vmem((firms, 2 * LANES), bf16),
        vmem((2 * LANES, rb * rows), bf16),
        vmem((ITERS, rb, tiles, LANES), f32),
        vmem((ITERS, rb, tiles, LANES), f32),
        vmem((ITERS, groups, qr, LANES), f32),
        vmem((ITERS, groups, qr, LANES), f32),
        vmem((ITERS - 1, groups, qr, LANES), f32),
        vmem((ITERS, 1, LANES), f32),
        vmem((ITERS, mkt * grp - 1, 1, LANES), f32),
        vmem((rb, owned, LANES), f32),
        vmem((rb, owned, LANES), f32),
        vmem((rb, owned, LANES), f32),
        vmem((rb, owned, LANES), f32),
        dma((11,)),
        dma((2, rb)), dma((2, rb)), dma((2, rb)), dma((2, rb)),
        dma((ITERS - 1, 2, rb)),
        dma((2, groups)), dma((2, groups)),
        dma((ITERS, 2, rb)),
        dma((ITERS, 2, groups)),
        dma((ITERS - 1, 2, groups)),
        dma((2, rb)), dma((2, rb)),
        dma((2, ITERS)),
    ]
    return pl.pallas_call(
        functools.partial(kernel, dims),
        out_shape=(
            jax.ShapeDtypeStruct((n_m, J), f32),
            jax.ShapeDtypeStruct((owned, R), f32),
        ),
        in_specs=[pl.BlockSpec(memory_space=pl.ANY)] * 11,
        out_specs=(spec, spec),
        scratch_shapes=scratch,
        compiler_params=pltpu.CompilerParams(
            collective_id=0, has_side_effects=True, vmem_limit_bytes=60 * 1024 * 1024
        ),
    )(
        market_size, taste_scale, taste_draws.transpose(1, 0, 2).reshape(n_m * K, R), type_weight,
        product_traits.transpose(2, 0, 1), product_firm, mean_utility, market_share,
        loyalty, firm_order.reshape(firms // LANES, LANES), firm_share,
    )


def solution(mesh):
    both = ("mkt", "grp")
    placed = (
        P(both, None), P(both, None), P(both, None, None), P(both, None, None), P(),
        P(both, None), P(both), P(both, None), P(), P(both, None), P(),
    )
    return jax.shard_map(
        functools.partial(local, mesh.shape["mkt"], mesh.shape["grp"]),
        mesh=mesh,
        in_specs=placed,
        out_specs=(P(both, None), P(both, None)),
        check_vma=False,
    )
```

```python
import functools

import jax
import jax.numpy as jnp
from jax import lax
from jax.experimental import pallas as pl
from jax.experimental.pallas import tpu as pltpu
from jax.sharding import PartitionSpec as P

ITERS = 3
FLAGS = 11 + 6 * ITERS + 5 * (ITERS - 1)
LANES = 128
MESH = pl.DeviceIdType.MESH

clip_target = 0.5
norm_eps = 1e-06

scope = jax.named_scope


def columns(row):
    return jnp.broadcast_to(row, (LANES, LANES)).T


def split_hi_lo(x):
    hi = x.astype(jnp.bfloat16)
    lo = (x - hi.astype(jnp.float32)).astype(jnp.bfloat16)
    return hi, lo


def xor(x, d, size):
    out = x
    bit = 1
    while bit < size:
        out = out + ((d // bit) % 2) * (1 - 2 * ((x // bit) % 2)) * bit
        bit *= 2
    return out


def kernel(
    dims,
    size_h, scale_h, draws_h, weight_h, traits_h, firm_h, mean_h, share_own_h, loy_h, order_h, share_h,
    mean_out, loy_out,
    size_ref, scale_ref, weight_ref, traits_ref, firm_ref, mean_ref, share_own_ref, order_ref, share_v,
    blk, loy, means, tbl, tq, tmass, tm_own,
    mass_own, lmat, rmat, one_hot, util, near_gap, col, order_col, order_row, table_hl, weighted_e, weighted_o,
    acc_e, acc_o,
    sums, sums_in, totals, totals_in, gap, squares, squares_in, old, old_in, last, last_in,
    in_s, blk_s, sem,
):
    mkt, grp, rb, groups, n_m, J, K, firms, owned, R = dims
    n = mkt * grp
    rows = n_m * J
    tiles = rows // LANES
    pair = LANES // J
    qr = firms // groups
    half = groups // 2
    near = half * qr
    pairs = rb // 2
    a = lax.axis_index("mkt")
    b = lax.axis_index("grp")
    ao, ai = a // rb, a % rb
    q_me = ao * grp + b
    me = a * grp + b

    def type_lane(d):
        return xor(ai, d, rb)

    def type_device(d):
        return (ao * rb + xor(ai, d, rb), b)

    def market_device(j):
        q = xor(q_me, j, groups)
        return ((q // grp) * rb + ai, q % grp)

    def lanes_of(p):
        return pl.ds(pl.multiple_of(p * LANES, LANES), LANES)

    names = {}

    def flag(*key):
        return sem.at[names.setdefault(key, len(names))]

    def send(src, dst, out_sem, in_sem, device):
        pltpu.make_async_remote_copy(
            src_ref=src, dst_ref=dst, send_sem=out_sem, recv_sem=in_sem, device_id=device, device_id_type=MESH,
        ).start()

    def arrive(ref, in_sem):
        pltpu.make_async_copy(ref, ref, in_sem).wait()

    m0 = n_m * K
    f0 = m0 + n_m

    def info_row(d, k, i):
        at = f0 + k * tiles + i
        return blk[d, at:at + 1, :]

    def pack(x):
        return jnp.concatenate([x[i * tiles:(i + 1) * tiles, :] for i in range(pair)], axis=1)

    inputs = {}
    for at, (key, src, dst) in enumerate((
        ("weight", weight_h, weight_ref), ("traits", traits_h, traits_ref), ("firm", firm_h, firm_ref),
        ("mean", mean_h, mean_ref), ("size", size_h, size_ref), ("scale", scale_h, scale_ref),
        ("draws", draws_h.at[:, lanes_of(ai)], blk.at[0, :m0]), ("loy", loy_h.at[:, lanes_of(ai)], loy.at[0]),
        ("order", order_h, order_ref), ("share_own", share_own_h, share_own_ref),
        ("share", share_h.at[:, lanes_of(ai)], share_v),
    )):
        inputs[key] = pltpu.make_async_copy(src, dst, in_s.at[at])
        inputs[key].start()

    barrier = pltpu.get_barrier_semaphore()

    @pl.loop(1, n)
    def _(d):
        t = (me + d) % n
        pl.semaphore_signal(barrier, inc=1, device_id=(t // grp, t % grp), device_id_type=MESH)

    for key in ("weight", "traits", "firm", "mean", "size", "scale"):
        inputs[key].wait()
    for k in range(K):
        blk[0, f0 + k * tiles:f0 + (k + 1) * tiles, :] = pack(traits_ref[k] * scale_ref[k])
    blk[0, f0 + K * tiles:f0 + (K + 1) * tiles, :] = pack(firm_ref[...].astype(jnp.float32))
    mean_now = pack(mean_ref[...])
    blk[0, f0 + (K + 1) * tiles:, :] = mean_now
    for m in range(n_m):
        mass_own[m:m + 1, :] = weight_ref[m:m + 1, :] * size_ref[m]

    with scope("bar"):
        pl.semaphore_wait(barrier, n - 1)

    for d in range(1, rb):
        send(loy_h.at[:, lanes_of(type_lane(d))], loy.at[d], flag("loy", 0), flag("loy", 1), type_device(d))
    for d in range(1, rb):
        device = type_device(d)
        lanes = lanes_of(type_lane(d))
        send(draws_h.at[:, lanes], blk.at[d, :m0], flag("blk", 0), blk_s.at[d], device)
        send(blk.at[0, f0:], blk.at[d, f0:], flag("blk", 0), blk_s.at[d], device)
        send(mass_own.at[:, lanes], blk.at[d, m0:f0], flag("blk", 0), blk_s.at[d], device)

    blk[0, m0:f0, :] = mass_own[:, lanes_of(ai)]
    weighted_o[:, (pairs - 1) * rows:] = jnp.zeros_like(weighted_o[:, (pairs - 1) * rows:])
    acc_e[...] = jnp.zeros_like(acc_e)
    acc_o[...] = jnp.zeros_like(acc_o)

    for key in ("order", "draws", "loy"):
        inputs[key].wait()
    for i in range(firms // LANES):
        col[i * LANES:(i + 1) * LANES, :] = columns(order_ref[i:i + 1, :].astype(jnp.float32))
    for j in range(groups):
        q = xor(q_me, j, groups)
        for d in range(rb):
            src = (((q // grp) * rb + xor(ai, d, rb)) * grp + q % grp) * owned
            dst = (j * rb + d) * owned
            order_col[dst:dst + owned, :] = col[pl.ds(pl.multiple_of(src, owned), owned), :]
    for i in range(firms // LANES):
        order_row[0:1, i * LANES:(i + 1) * LANES] = order_col[i * LANES:(i + 1) * LANES, :].T[0:1, :]

    kk = n_m * K
    row = lax.broadcasted_iota(jnp.int32, (n_m, LANES), 0)
    lane = lax.broadcasted_iota(jnp.int32, (n_m, LANES), 1)
    offset = row - (lane // J) * tiles
    zero = jnp.zeros((n_m, LANES), jnp.float32)
    rmat[kk:, :] = jnp.zeros_like(rmat[kk:, :])
    rmat[2 * kk:, :LANES] = jnp.ones_like(rmat[2 * kk:, :LANES])

    weighted = (weighted_e, weighted_o)

    def rows_of(d, r0, count):
        return pl.ds(pl.multiple_of(((d % 2) * pairs + d // 2) * rows + r0, LANES), count)

    def spread(part, where):
        return jnp.where(where, jnp.broadcast_to(part.astype(jnp.float32), (n_m, LANES)), zero).astype(jnp.bfloat16)

    def prepare(d):
        hi, lo = split_hi_lo(blk[d, :m0, :])
        rmat[:kk, :LANES] = hi
        rmat[:kk, LANES:] = lo
        rmat[kk:2 * kk, :LANES] = hi
        for i in range(tiles):
            here = offset == i
            at = slice(i * LANES, (i + 1) * LANES)
            for k in range(K):
                hi, lo = split_hi_lo(info_row(d, k, i))
                lmat[k * n_m:(k + 1) * n_m, at] = spread(hi, here)
                lmat[kk + k * n_m:kk + (k + 1) * n_m, at] = spread(lo, here)
            rest = info_row(d, K + 1, i)
            for s in range(3):
                hi = rest.astype(jnp.bfloat16)
                rest = rest - hi.astype(jnp.float32)
                lmat[2 * kk + s * n_m:2 * kk + (s + 1) * n_m, at] = spread(hi, here)
        both = lax.dot_general(
            lmat[...], rmat[...], (((0,), (0,)), ((), ())), preferred_element_type=jnp.float32
        )
        util[rows_of(d, 0, rows), :] = both[:, :LANES] + both[:, LANES:]
        for i in range(tiles):
            firm_col = columns(info_row(d, K, i))
            for f in range(firms // LANES):
                one_hot[rows_of(d, i * LANES, LANES), f * LANES:(f + 1) * LANES] = (
                    firm_col == order_row[0:1, f * LANES:(f + 1) * LANES]
                ).astype(jnp.float32).astype(jnp.bfloat16)

    with scope("prep0"):
        prepare(0)

    with scope("arr_loy"):
        arrive(loy.at[1:], flag("loy", 1))
    for d in range(rb):
        tq[d * owned:(d + 1) * owned, :] = loy[d]
    for j in range(1, groups):
        send(tq, tbl.at[j], flag("tq", 0), flag("tq", 1), market_device(j))
    tbl[0] = tq[...]

    def arrive_inputs(d):
        arrive(blk.at[d], blk_s.at[d])

    first = rb // 2

    @pl.loop(1, first)
    def _(d):
        with scope("arr_a"):
            arrive_inputs(d)
        with scope("prep_a"):
            prepare(d)

    with scope("share"):
        inputs["share"].wait()
        inputs["share_own"].wait()
        mine_col = order_col[:qr, :]
        number = lax.broadcasted_iota(jnp.int32, (qr, LANES), 1).astype(jnp.float32)
        my_share = jnp.zeros((qr, LANES), jnp.float32)
        for i in range(firms // LANES):
            pick = (mine_col == number + float(i * LANES)).astype(jnp.float32)
            my_share += jnp.dot(
                pick, share_v[i * LANES:(i + 1) * LANES, :],
                precision=lax.Precision.HIGHEST, preferred_element_type=jnp.float32,
            )
        my_share = jnp.log(my_share)
        base = jnp.log(share_own_ref[...]) + jnp.log(jnp.sum(mass_own[...], axis=1, keepdims=True))
        base = pack(base)

    with scope("arr_tbl"):
        arrive(tbl.at[1:], flag("tq", 1))

    def split_into(j, value):
        hi, lo = split_hi_lo(value)
        table_hl[j * qr:(j + 1) * qr, :LANES] = hi
        table_hl[j * qr:(j + 1) * qr, LANES:] = lo

    for j in range(groups):
        split_into(j, tbl[j])

    per_block = 2
    block = per_block * LANES

    def gather(d, r0, begin, end):
        both = jnp.dot(
            one_hot[rows_of(d, r0, block), begin:end], table_hl[begin:end, :], preferred_element_type=jnp.float32
        )
        return both[:, :LANES] + both[:, LANES:]

    def shares(it, i, par, clip, other):
        d = 2 * i + par
        moved = None
        for h in range(rows // block):
            r0 = h * block
            at = rows_of(d, r0, block)
            if it == 0:
                u = util[at, :] + gather(d, r0, 0, firms)
            else:
                u = util[at, :] + clip * (near_gap[at, :] + gather(d, r0, near, firms))
            if it < ITERS - 1:
                util[at, :] = u
            chunk = far_part(other, 1 - par, r0, block)
            moved = chunk if moved is None else moved + chunk
            expu = jnp.exp(u)
            for c in range(per_block):
                t = h * per_block + c
                parts = []
                for s in range(pair):
                    part = expu[c * LANES + s * J:c * LANES + (s + 1) * J, :]
                    m = s * tiles + t
                    parts.append(
                        part * (blk[d, m0 + m:m0 + m + 1, :] / (1.0 + jnp.sum(part, axis=0, keepdims=True)))
                    )
                bought = jnp.concatenate(parts, axis=0).T
                sums[it, d, t:t + 1, :] = jnp.sum(bought, axis=0, keepdims=True)
                hi, lo = split_hi_lo(bought)
                lanes = pl.ds(pl.multiple_of(i * rows + t * LANES, LANES), LANES)
                weighted[par][:LANES, lanes] = hi
                weighted[par][LANES:, lanes] = lo
        return moved

    def far_part(i, par, r0, count):
        lanes = pl.ds(pl.multiple_of(i * rows + r0, LANES), count)
        part = jnp.dot(
            weighted[par][:, lanes], one_hot[rows_of(2 * i + par, r0, count), near:],
            preferred_element_type=jnp.float32,
        )
        return part[:LANES, :] + part[LANES:, :]

    def pair_step(it, s, clip, ready):
        i = s if it == 0 else pairs - 1 - s
        prev = (s + pairs - 1) % pairs if it == 0 else (pairs - s) % pairs
        started = s > 0
        ready(2 * i)
        part = shares(it, i, 0, clip, prev)
        acc_o[...] = jnp.where(started, acc_o[...] + part, 0.0)
        ready(2 * i + 1)
        part = shares(it, i, 1, clip, i)
        acc_e[...] = jnp.where(started, acc_e[...], 0.0) + part
        send_sums(it, 2 * i + 1)

        @pl.when(i > 0)
        def _():
            send_sums(it, 2 * i)

    def send_sums(it, d):
        send(sums.at[it, d], sums_in.at[it, d], flag("sums", it, 0), flag("sums", it, 1), type_device(d))

    def by_firm(x):
        return jnp.concatenate([x[:, i * LANES:(i + 1) * LANES].T for i in range(near // LANES)], axis=0)

    def far_totals(it):
        acc = by_firm(acc_e[...] + acc_o[...] + far_part(pairs - 1 if it == 0 else 0, 1, 0, rows))
        for j in range(half):
            totals[it, half + j] = acc[j * qr:(j + 1) * qr, :]

    def near_totals(it):
        acc = None
        for par in range(2):
            part = jnp.dot(
                weighted[par][...], one_hot[par * pairs * rows:(par + 1) * pairs * rows, :near],
                preferred_element_type=jnp.float32,
            )
            part = by_firm(part[:LANES, :] + part[LANES:, :])
            acc = part if acc is None else acc + part
        for j in range(half):
            totals[it, j] = acc[j * qr:(j + 1) * qr, :]

    clip = None
    log_mass = None
    for it in range(ITERS):
        final = it == ITERS - 1
        if it == 0:
            with scope("sh_a"):
                @pl.loop(0, first // 2)
                def _(i):
                    pair_step(0, i, None, lambda d: None)

            def ready(d):
                with scope("arr_b"):
                    arrive_inputs(d)
                prepare(d)

            @pl.loop(first // 2, pairs)
            def _(i):
                pair_step(0, i, None, ready)

            tm_own[...] = jnp.zeros_like(tm_own)
            for d in range(rb):
                tm_own[...] += jnp.sum(blk[d, m0:f0, :], axis=0, keepdims=True)
            for j in range(1, groups):
                send(tm_own, tmass.at[j], flag("tm", 0), flag("tm", 1), market_device(j))
            tmass[0] = tm_own[...]
        else:
            with scope("shares%d" % it):
                @pl.loop(0, pairs)
                def _(i):
                    pair_step(it, i, clip, lambda d: None)

        sums_in[it, 0] = sums[it, 0]

        with scope("far%d" % it):
            far_totals(it)
        for j in range(half, groups):
            send(totals.at[it, j], totals_in.at[it, j], flag("totals", it, 0), flag("totals", it, 1), market_device(j))
        with scope("near%d" % it):
            near_totals(it)
        for j in range(1, half):
            send(totals.at[it, j], totals_in.at[it, j], flag("totals", it, 0), flag("totals", it, 1), market_device(j))
        totals_in[it, 0] = totals[it, 0]

        if final:
            for d in range(rb):
                old[d] = tbl[0, d * owned:(d + 1) * owned, :]
            for d in range(1, rb):
                send(old.at[d], old_in.at[d], flag("old", 0), flag("old", 1), type_device(d))
            old_in[0] = old[0]

        if it == 0:
            arrive(tmass.at[1:], flag("tm", 1))
            log_mass = jnp.log(jnp.sum(tmass[...], axis=0))

        def settle_means(mean_now):
            with scope("arr_sums%d" % it):
                arrive(sums_in.at[it, 1:], flag("sums", it, 1))
            step = base - jnp.log(jnp.sum(sums_in[it], axis=0))
            mean_now = mean_now + step
            if final:
                for i in range(pair):
                    mean_out[i * tiles:(i + 1) * tiles, :] = mean_now[:, i * J:(i + 1) * J]
            else:
                means[it, 0] = step
                for d in range(1, rb):
                    send(means.at[it, 0], means.at[it, d], flag("means", it, 0), flag("means", it, 1), type_device(d))
            return mean_now

        if it:
            mean_now = settle_means(mean_now)
        with scope("arr_tot%d" % it):
            arrive(totals_in.at[it, 1:], flag("totals", it, 1))
        gap_mine = my_share - (jnp.log(jnp.sum(totals_in[it], axis=0)) - log_mass)
        squares[it] = jnp.sum(gap_mine * gap_mine, axis=0, keepdims=True)

        @pl.loop(1, n)
        def _(d):
            t = (me + d) % n
            send(
                squares.at[it], squares_in.at[it, d - 1], flag("sq", it, 0), flag("sq", it, 1), (t // grp, t % grp)
            )

        if final:
            for d in range(rb):
                last[d] = gap_mine[d * owned:(d + 1) * owned, :]
            for d in range(1, rb):
                send(last.at[d], last_in.at[d], flag("last", 0), flag("last", 1), type_device(d))
            last_in[0] = last[0]
        else:
            gap[it, 0] = gap_mine
            for j in [*range(half, groups), *range(1, half)]:
                send(gap.at[it, 0], gap.at[it, j], flag("gap", it, 0), flag("gap", it, 1 + j // half), market_device(j))
            if it == 0:
                mean_now = settle_means(mean_now)
            with scope("arr_gapn%d" % it):
                split_into(0, gap_mine)
                arrive(gap.at[it, 1:half], flag("gap", it, 1))
                for j in range(1, half):
                    split_into(j, gap[it, j])

            with scope("gnear%d" % it):
                @pl.loop(0, pairs)
                def _(i):
                    for par in range(2):
                        at = rows_of(2 * i + par, 0, rows)
                        both = jnp.dot(one_hot[at, :near], table_hl[:near, :], preferred_element_type=jnp.float32)
                        near_gap[at, :] = both[:, :LANES] + both[:, LANES:]

            with scope("arr_mean%d" % it):
                arrive(means.at[it, 1:], flag("means", it, 1))

            with scope("addmean%d" % it):
                @pl.loop(0, pairs)
                def _(i):
                    for par in range(2):
                        for t in range(tiles):
                            at = rows_of(2 * i + par, t * LANES, LANES)
                            util[at, :] = util[at, :] + columns(means[it, 2 * i + par, t:t + 1, :])

            with scope("arr_gap%d" % it):
                arrive(gap.at[it, half:], flag("gap", it, 2))
                for j in range(half, groups):
                    split_into(j, gap[it, j])

        with scope("arr_sq%d" % it):
            arrive(squares_in.at[it], flag("sq", it, 1))
        total = jnp.sum(jnp.sum(squares_in[it], axis=0) + squares[it], axis=1, keepdims=True)
        clip = jnp.minimum(1.0, clip_target / jnp.sqrt(total / (firms * R) + norm_eps))

        if final:
            with scope("arr_last"):
                arrive(old_in.at[1:], flag("old", 1))
                arrive(last_in.at[1:], flag("last", 1))
            for d in range(rb):
                loy_out[:, lanes_of(type_lane(d))] = old_in[d] + clip * last_in[d]
        else:
            tbl[0] = tbl[0] + clip * gap_mine

    with scope("drain"):
        arrive(loy.at[1:], flag("loy", 0))
        arrive(blk.at[1:], flag("blk", 0))
        arrive(tbl.at[1:], flag("tq", 0))
        arrive(tmass.at[1:], flag("tm", 0))
        arrive(old.at[1:], flag("old", 0))
        arrive(last.at[1:], flag("last", 0))
        for it in range(ITERS):
            arrive(sums.at[it, 1:], flag("sums", it, 0))
            arrive(totals.at[it, 1:], flag("totals", it, 0))
            arrive(squares_in.at[it], flag("sq", it, 0))
            if it < ITERS - 1:
                arrive(means.at[it, 1:], flag("means", it, 0))
                arrive(gap.at[it, 1:], flag("gap", it, 0))
    assert len(names) == FLAGS


def local(
    mkt, grp,
    mean_utility, market_share, product_traits, taste_draws, taste_scale, type_weight,
    market_size, product_firm, firm_order, loyalty, firm_share,
):
    n_m, J, K = product_traits.shape
    firms, R = firm_share.shape
    owned = loyalty.shape[0]
    rb = R // LANES
    groups = mkt * grp // rb
    rows = n_m * J
    tiles = rows // LANES
    qr = firms // groups
    depth = n_m * (2 * K + 3)

    f32, bf16 = jnp.float32, jnp.bfloat16
    dma = pltpu.SemaphoreType.DMA
    vmem = pltpu.VMEM
    spec = pl.BlockSpec(memory_space=pltpu.VMEM)
    dims = (mkt, grp, rb, groups, n_m, J, K, firms, owned, R)
    scratch = [
        pltpu.SMEM((n_m,), f32),
        pltpu.SMEM((K,), f32),
        vmem((n_m, R), f32),
        vmem((K, n_m, J), f32),
        vmem((n_m, J), jnp.int32),
        vmem((n_m, J), f32),
        vmem((n_m, J), f32),
        vmem((firms // LANES, LANES), jnp.int32),
        vmem((firms, LANES), f32),
        vmem((rb, n_m * (K + 1) + (K + 2) * tiles, LANES), f32),
        vmem((rb, owned, LANES), f32),
        vmem((ITERS - 1, rb, tiles, LANES), f32),
        vmem((groups, qr, LANES), f32),
        vmem((qr, LANES), f32),
        vmem((groups, 1, LANES), f32),
        vmem((1, LANES), f32),
        vmem((n_m, R), f32),
        vmem((depth, rows), bf16),
        vmem((depth, 2 * LANES), bf16),
        vmem((rb * rows, firms), bf16),
        vmem((rb * rows, LANES), f32),
        vmem((rb * rows, LANES), f32),
        vmem((firms, LANES), f32),
        vmem((firms, LANES), f32),
        vmem((1, firms), f32),
        vmem((firms, 2 * LANES), bf16),
        vmem((2 * LANES, rb // 2 * rows), bf16),
        vmem((2 * LANES, rb // 2 * rows), bf16),
        vmem((LANES, firms // 2), f32),
        vmem((LANES, firms // 2), f32),
        vmem((ITERS, rb, tiles, LANES), f32),
        vmem((ITERS, rb, tiles, LANES), f32),
        vmem((ITERS, groups, qr, LANES), f32),
        vmem((ITERS, groups, qr, LANES), f32),
        vmem((ITERS - 1, groups, qr, LANES), f32),
        vmem((ITERS, 1, LANES), f32),
        vmem((ITERS, mkt * grp - 1, 1, LANES), f32),
        vmem((rb, owned, LANES), f32),
        vmem((rb, owned, LANES), f32),
        vmem((rb, owned, LANES), f32),
        vmem((rb, owned, LANES), f32),
        dma((11,)),
        dma((rb,)),
        dma((FLAGS,)),
    ]
    return pl.pallas_call(
        functools.partial(kernel, dims),
        out_shape=(
            jax.ShapeDtypeStruct((n_m, J), f32),
            jax.ShapeDtypeStruct((owned, R), f32),
        ),
        in_specs=[pl.BlockSpec(memory_space=pl.ANY)] * 11,
        out_specs=(spec, spec),
        scratch_shapes=scratch,
        compiler_params=pltpu.CompilerParams(
            collective_id=0, has_side_effects=True, vmem_limit_bytes=60 * 1024 * 1024
        ),
    )(
        market_size, taste_scale, taste_draws.transpose(1, 0, 2).reshape(n_m * K, R), type_weight,
        product_traits.transpose(2, 0, 1), product_firm, mean_utility, market_share,
        loyalty, firm_order.reshape(firms // LANES, LANES), firm_share,
    )


def solution(mesh):
    both = ("mkt", "grp")
    placed = (
        P(both, None), P(both, None), P(both, None, None), P(both, None, None), P(),
        P(both, None), P(both), P(both, None), P(), P(both, None), P(),
    )
    return jax.shard_map(
        functools.partial(local, mesh.shape["mkt"], mesh.shape["grp"]),
        mesh=mesh,
        in_specs=placed,
        out_specs=(P(both, None), P(both, None)),
        check_vma=False,
    )
```

```python
import functools

import jax
import jax.numpy as jnp
from jax import lax
from jax.experimental import pallas as pl
from jax.experimental.pallas import tpu as pltpu
from jax.sharding import PartitionSpec as P

ITERS = 3
FLAGS = 12 + 6 * ITERS + 5 * (ITERS - 1)
LANES = 128
MESH = pl.DeviceIdType.MESH

clip_target = 0.5
norm_eps = 1e-06

scope = jax.named_scope


def columns(row):
    return jnp.broadcast_to(row, (LANES, LANES)).T


def split_hi_lo(x):
    hi = x.astype(jnp.bfloat16)
    lo = (x - hi.astype(jnp.float32)).astype(jnp.bfloat16)
    return hi, lo


def xor(x, d, size):
    out = x
    bit = 1
    while bit < size:
        out = out + ((d // bit) % 2) * (1 - 2 * ((x // bit) % 2)) * bit
        bit *= 2
    return out


def kernel(
    dims,
    size_h, scale_h, draws_h, weight_h, traits_h, firm_h, mean_h, share_own_h, loy_h, order_h, share_h,
    mean_out, loy_out,
    size_ref, scale_ref, weight_ref, traits_ref, firm_ref, mean_ref, share_own_ref, order_ref, share_v,
    blk, info, loy, means, tbl, tq, tmass, tm_own,
    mass_own, lmat, rmats, one_hot, util, near_gap, col, order_col, order_row, table_hl, weighted_e, weighted_o,
    acc_e, acc_o,
    sums, sums_in, totals, totals_in, gap, squares, squares_in, old, old_in, last, last_in,
    in_s, blk_s, info_s, sem,
):
    mkt, grp, rb, groups, n_m, J, K, firms, owned, R = dims
    n = mkt * grp
    rows = n_m * J
    tiles = rows // LANES
    pair = LANES // J
    qr = firms // groups
    half = groups // 2
    near = half * qr
    pairs = rb // 2
    a = lax.axis_index("mkt")
    b = lax.axis_index("grp")
    ao, ai = a // rb, a % rb
    q_me = ao * grp + b
    me = a * grp + b

    def type_lane(d):
        return xor(ai, d, rb)

    def type_device(d):
        return (ao * rb + xor(ai, d, rb), b)

    def market_device(j):
        q = xor(q_me, j, groups)
        return ((q // grp) * rb + ai, q % grp)

    def lanes_of(p):
        return pl.ds(pl.multiple_of(p * LANES, LANES), LANES)

    names = {}

    def flag(*key):
        return sem.at[names.setdefault(key, len(names))]

    def send(src, dst, out_sem, in_sem, device):
        pltpu.make_async_remote_copy(
            src_ref=src, dst_ref=dst, send_sem=out_sem, recv_sem=in_sem, device_id=device, device_id_type=MESH,
        ).start()

    def arrive(ref, in_sem):
        pltpu.make_async_copy(ref, ref, in_sem).wait()

    m0 = n_m * K

    def info_row(d, k, i):
        at = k * tiles + i
        return info[d, at:at + 1, :]

    def pack(x):
        return jnp.concatenate([x[i * tiles:(i + 1) * tiles, :] for i in range(pair)], axis=1)

    inputs = {}
    for at, (key, src, dst) in enumerate((
        ("weight", weight_h, weight_ref), ("traits", traits_h, traits_ref), ("firm", firm_h, firm_ref),
        ("mean", mean_h, mean_ref), ("size", size_h, size_ref), ("scale", scale_h, scale_ref),
        ("draws", draws_h.at[:, lanes_of(ai)], blk.at[0, :m0]), ("loy", loy_h.at[:, lanes_of(ai)], loy.at[0]),
        ("order", order_h, order_ref), ("share_own", share_own_h, share_own_ref),
        ("share", share_h.at[:, lanes_of(ai)], share_v),
    )):
        inputs[key] = pltpu.make_async_copy(src, dst, in_s.at[at])
        inputs[key].start()

    barrier = pltpu.get_barrier_semaphore()

    @pl.loop(1, n)
    def _(d):
        t = (me + d) % n
        pl.semaphore_signal(barrier, inc=1, device_id=(t // grp, t % grp), device_id_type=MESH)

    for key in ("weight", "traits", "firm", "mean", "size", "scale"):
        inputs[key].wait()
    for k in range(K):
        info[0, k * tiles:(k + 1) * tiles, :] = pack(traits_ref[k] * scale_ref[k])
    info[0, K * tiles:(K + 1) * tiles, :] = pack(firm_ref[...].astype(jnp.float32))
    mean_now = pack(mean_ref[...])
    info[0, (K + 1) * tiles:, :] = mean_now
    for m in range(n_m):
        mass_own[m:m + 1, :] = weight_ref[m:m + 1, :] * size_ref[m]

    with scope("bar"):
        pl.semaphore_wait(barrier, n - 1)

    for d in range(1, rb):
        send(loy_h.at[:, lanes_of(type_lane(d))], loy.at[d], flag("loy", 0), flag("loy", 1), type_device(d))
    for d in [1, *range(2, rb, 2)]:
        send(info.at[0], info.at[d], flag("info", 0), info_s.at[d], type_device(d))
    for d in range(1, rb):
        device = type_device(d)
        lanes = lanes_of(type_lane(d))
        send(draws_h.at[:, lanes], blk.at[d, :m0], flag("blk", 0), blk_s.at[d], device)
        send(mass_own.at[:, lanes], blk.at[d, m0:], flag("blk", 0), blk_s.at[d], device)

    def arrive_info(d):
        arrive(info.at[d], info_s.at[d])

    def hand_on(d):
        send(info.at[d], info.at[d + 1], flag("info", 0), info_s.at[d + 1], type_device(1))

    blk[0, m0:, :] = mass_own[:, lanes_of(ai)]
    weighted_o[:, (pairs - 1) * rows:] = jnp.zeros_like(weighted_o[:, (pairs - 1) * rows:])
    acc_e[...] = jnp.zeros_like(acc_e)
    acc_o[...] = jnp.zeros_like(acc_o)

    for key in ("order", "draws", "loy"):
        inputs[key].wait()
    for i in range(firms // LANES):
        col[i * LANES:(i + 1) * LANES, :] = columns(order_ref[i:i + 1, :].astype(jnp.float32))
    for j in range(groups):
        q = xor(q_me, j, groups)
        for d in range(rb):
            src = (((q // grp) * rb + xor(ai, d, rb)) * grp + q % grp) * owned
            dst = (j * rb + d) * owned
            order_col[dst:dst + owned, :] = col[pl.ds(pl.multiple_of(src, owned), owned), :]
    for i in range(firms // LANES):
        order_row[0:1, i * LANES:(i + 1) * LANES] = order_col[i * LANES:(i + 1) * LANES, :].T[0:1, :]

    kk = n_m * K
    row = lax.broadcasted_iota(jnp.int32, (n_m, LANES), 0)
    lane = lax.broadcasted_iota(jnp.int32, (n_m, LANES), 1)
    offset = row - (lane // J) * tiles
    zero = jnp.zeros((n_m, LANES), jnp.float32)
    rmats[:, kk:, :] = jnp.zeros_like(rmats[:, kk:, :])
    rmats[:, 2 * kk:, :LANES] = jnp.ones_like(rmats[:, 2 * kk:, :LANES])

    weighted = (weighted_e, weighted_o)

    def rows_of(d, r0, count):
        return pl.ds(pl.multiple_of(((d % 2) * pairs + d // 2) * rows + r0, LANES), count)

    def spread(part, where):
        return jnp.where(where, jnp.broadcast_to(part.astype(jnp.float32), (n_m, LANES)), zero).astype(jnp.bfloat16)

    def build(d):
        for i in range(tiles):
            here = offset == i
            at = slice(i * LANES, (i + 1) * LANES)
            for k in range(K):
                hi, lo = split_hi_lo(info_row(d, k, i))
                lmat[d, k * n_m:(k + 1) * n_m, at] = spread(hi, here)
                lmat[d, kk + k * n_m:kk + (k + 1) * n_m, at] = spread(lo, here)
            rest = info_row(d, K + 1, i)
            for s in range(3):
                hi = rest.astype(jnp.bfloat16)
                rest = rest - hi.astype(jnp.float32)
                lmat[d, 2 * kk + s * n_m:2 * kk + (s + 1) * n_m, at] = spread(hi, here)
        for i in range(tiles):
            firm_col = columns(info_row(d, K, i))
            for f in range(firms // LANES):
                one_hot[rows_of(d, i * LANES, LANES), f * LANES:(f + 1) * LANES] = (
                    firm_col == order_row[0:1, f * LANES:(f + 1) * LANES]
                ).astype(jnp.float32).astype(jnp.bfloat16)

    def taste(d, par):
        rmat = rmats.at[par]
        hi, lo = split_hi_lo(blk[d, :m0, :])
        rmat[:kk, :LANES] = hi
        rmat[:kk, LANES:] = lo
        rmat[kk:2 * kk, :LANES] = hi
        both = lax.dot_general(
            lmat[d], rmat[...], (((0,), (0,)), ((), ())), preferred_element_type=jnp.float32
        )
        util[rows_of(d, 0, rows), :] = both[:, :LANES] + both[:, LANES:]

    with scope("prep0"):
        build(0)
        taste(0, 0)
    with scope("share"):
        inputs["share"].wait()
        inputs["share_own"].wait()
        mine_col = order_col[:qr, :]
        number = lax.broadcasted_iota(jnp.int32, (qr, LANES), 1).astype(jnp.float32)
        my_share = jnp.zeros((qr, LANES), jnp.float32)
        for i in range(firms // LANES):
            pick = (mine_col == number + float(i * LANES)).astype(jnp.float32)
            my_share += jnp.dot(
                pick, share_v[i * LANES:(i + 1) * LANES, :],
                precision=lax.Precision.HIGHEST, preferred_element_type=jnp.float32,
            )
        my_share = jnp.log(my_share)
        base = jnp.log(share_own_ref[...]) + jnp.log(jnp.sum(mass_own[...], axis=1, keepdims=True))
        base = pack(base)

    with scope("arr_i2"):
        arrive_info(2)
    hand_on(2)
    with scope("arr_i1"):
        arrive_info(1)

    @pl.loop(1, 3)
    def _(d):
        with scope("build12"):
            build(d)

    with scope("arr_loy"):
        arrive(loy.at[1:], flag("loy", 1))
    for d in range(rb):
        tq[d * owned:(d + 1) * owned, :] = loy[d]
    for j in range(1, groups):
        send(tq, tbl.at[j], flag("tq", 0), flag("tq", 1), market_device(j))
    tbl[0] = tq[...]

    @pl.loop(2, pairs)
    def _(i):
        with scope("arr_ie"):
            arrive_info(2 * i)
        hand_on(2 * i)
        build(2 * i)

    @pl.loop(1, pairs)
    def _(i):
        with scope("arr_io"):
            arrive_info(2 * i + 1)
        build(2 * i + 1)

    def arrive_inputs(d):
        arrive(blk.at[d], blk_s.at[d])

    first = rb // 2

    @pl.loop(1, first)
    def _(d):
        with scope("arr_a"):
            arrive_inputs(d)
        with scope("prep_a"):
            taste(d, 0)

    with scope("arr_tbl"):
        arrive(tbl.at[1:], flag("tq", 1))

    def split_into(j, value):
        hi, lo = split_hi_lo(value)
        table_hl[j * qr:(j + 1) * qr, :LANES] = hi
        table_hl[j * qr:(j + 1) * qr, LANES:] = lo

    for j in range(groups):
        split_into(j, tbl[j])

    per_block = 2
    block = per_block * LANES

    def gather(d, r0, begin, end):
        both = jnp.dot(
            one_hot[rows_of(d, r0, block), begin:end], table_hl[begin:end, :], preferred_element_type=jnp.float32
        )
        return both[:, :LANES] + both[:, LANES:]

    def shares(it, i, par, clip, other):
        d = 2 * i + par
        moved = None
        for h in range(rows // block):
            r0 = h * block
            at = rows_of(d, r0, block)
            if it == 0:
                u = util[at, :] + gather(d, r0, 0, firms)
            else:
                u = util[at, :] + clip * (near_gap[at, :] + gather(d, r0, near, firms))
            if it < ITERS - 1:
                util[at, :] = u
            chunk = far_part(other, 1 - par, r0, block)
            moved = chunk if moved is None else moved + chunk
            expu = jnp.exp(u)
            for c in range(per_block):
                t = h * per_block + c
                parts = []
                for s in range(pair):
                    part = expu[c * LANES + s * J:c * LANES + (s + 1) * J, :]
                    m = s * tiles + t
                    parts.append(
                        part * (blk[d, m0 + m:m0 + m + 1, :] / (1.0 + jnp.sum(part, axis=0, keepdims=True)))
                    )
                bought = jnp.concatenate(parts, axis=0).T
                sums[it, d, t:t + 1, :] = jnp.sum(bought, axis=0, keepdims=True)
                hi, lo = split_hi_lo(bought)
                lanes = pl.ds(pl.multiple_of(i * rows + t * LANES, LANES), LANES)
                weighted[par][:LANES, lanes] = hi
                weighted[par][LANES:, lanes] = lo
        return moved

    def far_part(i, par, r0, count):
        lanes = pl.ds(pl.multiple_of(i * rows + r0, LANES), count)
        part = jnp.dot(
            weighted[par][:, lanes], one_hot[rows_of(2 * i + par, r0, count), near:],
            preferred_element_type=jnp.float32,
        )
        return part[:LANES, :] + part[LANES:, :]

    def pair_step(it, s, clip, ready):
        i = s if it == 0 else pairs - 1 - s
        prev = (s + pairs - 1) % pairs if it == 0 else (pairs - s) % pairs
        started = s > 0
        ready(i)
        part = shares(it, i, 0, clip, prev)
        acc_o[...] = jnp.where(started, acc_o[...] + part, 0.0)
        part = shares(it, i, 1, clip, i)
        acc_e[...] = jnp.where(started, acc_e[...], 0.0) + part
        send_sums(it, 2 * i + 1)

        if isinstance(i, int):
            if i:
                send_sums(it, 2 * i)
        else:
            @pl.when(i > 0)
            def _():
                send_sums(it, 2 * i)

    def send_sums(it, d):
        send(sums.at[it, d], sums_in.at[it, d], flag("sums", it, 0), flag("sums", it, 1), type_device(d))

    def by_firm(x):
        return jnp.concatenate([x[:, i * LANES:(i + 1) * LANES].T for i in range(near // LANES)], axis=0)

    def far_totals(it):
        acc = by_firm(acc_e[...] + acc_o[...] + far_part(pairs - 1 if it == 0 else 0, 1, 0, rows))
        for j in range(half):
            totals[it, half + j] = acc[j * qr:(j + 1) * qr, :]

    def near_totals(it):
        acc = None
        for par in range(2):
            part = jnp.dot(
                weighted[par][...], one_hot[par * pairs * rows:(par + 1) * pairs * rows, :near],
                preferred_element_type=jnp.float32,
            )
            part = by_firm(part[:LANES, :] + part[LANES:, :])
            acc = part if acc is None else acc + part
        for j in range(half):
            totals[it, j] = acc[j * qr:(j + 1) * qr, :]

    clip = None
    log_mass = None
    for it in range(ITERS):
        final = it == ITERS - 1
        if it == 0:
            with scope("sh_a"):
                @pl.loop(0, first // 2)
                def _(i):
                    pair_step(0, i, None, lambda d: None)

            def ready(i):
                with scope("arr_b"):
                    for par in range(2):
                        arrive_inputs(2 * i + par)
                with scope("taste_b"):
                    for par in range(2):
                        taste(2 * i + par, par)

            @pl.loop(first // 2, pairs)
            def _(i):
                pair_step(0, i, None, ready)

            tm_own[...] = jnp.zeros_like(tm_own)
            for d in range(rb):
                tm_own[...] += jnp.sum(blk[d, m0:, :], axis=0, keepdims=True)
            for j in range(1, groups):
                send(tm_own, tmass.at[j], flag("tm", 0), flag("tm", 1), market_device(j))
            tmass[0] = tm_own[...]
        else:
            with scope("shares%d" % it):
                for i in range(pairs):
                    pair_step(it, i, clip, lambda d: None)

        sums_in[it, 0] = sums[it, 0]

        with scope("far%d" % it):
            far_totals(it)
        for j in range(half, groups):
            send(totals.at[it, j], totals_in.at[it, j], flag("totals", it, 0), flag("totals", it, 1), market_device(j))
        with scope("near%d" % it):
            near_totals(it)
        for j in range(1, half):
            send(totals.at[it, j], totals_in.at[it, j], flag("totals", it, 0), flag("totals", it, 1), market_device(j))
        totals_in[it, 0] = totals[it, 0]

        if final:
            for d in range(rb):
                old[d] = tbl[0, d * owned:(d + 1) * owned, :]
            for d in range(1, rb):
                send(old.at[d], old_in.at[d], flag("old", 0), flag("old", 1), type_device(d))
            old_in[0] = old[0]

        if it == 0:
            arrive(tmass.at[1:], flag("tm", 1))
            log_mass = jnp.log(jnp.sum(tmass[...], axis=0))

        def settle_means(mean_now):
            with scope("arr_sums%d" % it):
                arrive(sums_in.at[it, 1:], flag("sums", it, 1))
            step = base - jnp.log(jnp.sum(sums_in[it], axis=0))
            mean_now = mean_now + step
            if final:
                for i in range(pair):
                    mean_out[i * tiles:(i + 1) * tiles, :] = mean_now[:, i * J:(i + 1) * J]
            else:
                means[it, 0] = step
                for d in range(1, rb):
                    send(means.at[it, 0], means.at[it, d], flag("means", it, 0), flag("means", it, 1), type_device(d))
            return mean_now

        if it:
            mean_now = settle_means(mean_now)
        with scope("arr_tot%d" % it):
            arrive(totals_in.at[it, 1:], flag("totals", it, 1))
        gap_mine = my_share - (jnp.log(jnp.sum(totals_in[it], axis=0)) - log_mass)
        squares[it] = jnp.sum(gap_mine * gap_mine, axis=0, keepdims=True)

        @pl.loop(1, n)
        def _(d):
            t = (me + d) % n
            send(
                squares.at[it], squares_in.at[it, d - 1], flag("sq", it, 0), flag("sq", it, 1), (t // grp, t % grp)
            )

        if final:
            for d in range(rb):
                last[d] = gap_mine[d * owned:(d + 1) * owned, :]
            for d in range(1, rb):
                send(last.at[d], last_in.at[d], flag("last", 0), flag("last", 1), type_device(d))
            last_in[0] = last[0]
        else:
            gap[it, 0] = gap_mine
            for j in [*range(half, groups), *range(1, half)]:
                send(gap.at[it, 0], gap.at[it, j], flag("gap", it, 0), flag("gap", it, 1 + j // half), market_device(j))
            if it == 0:
                mean_now = settle_means(mean_now)
            with scope("arr_gapn%d" % it):
                split_into(0, gap_mine)
                arrive(gap.at[it, 1:half], flag("gap", it, 1))
                for j in range(1, half):
                    split_into(j, gap[it, j])

            with scope("gnear%d" % it):
                @pl.loop(0, pairs)
                def _(i):
                    for par in range(2):
                        at = rows_of(2 * i + par, 0, rows)
                        both = jnp.dot(one_hot[at, :near], table_hl[:near, :], preferred_element_type=jnp.float32)
                        near_gap[at, :] = both[:, :LANES] + both[:, LANES:]

            with scope("arr_mean%d" % it):
                arrive(means.at[it, 1:], flag("means", it, 1))

            with scope("addmean%d" % it):
                @pl.loop(0, pairs)
                def _(i):
                    for par in range(2):
                        for t in range(tiles):
                            at = rows_of(2 * i + par, t * LANES, LANES)
                            util[at, :] = util[at, :] + columns(means[it, 2 * i + par, t:t + 1, :])

            with scope("arr_gap%d" % it):
                arrive(gap.at[it, half:], flag("gap", it, 2))
                for j in range(half, groups):
                    split_into(j, gap[it, j])

        with scope("arr_sq%d" % it):
            arrive(squares_in.at[it], flag("sq", it, 1))
        total = jnp.sum(jnp.sum(squares_in[it], axis=0) + squares[it], axis=1, keepdims=True)
        clip = jnp.minimum(1.0, clip_target / jnp.sqrt(total / (firms * R) + norm_eps))

        if final:
            with scope("arr_last"):
                arrive(old_in.at[1:], flag("old", 1))
                arrive(last_in.at[1:], flag("last", 1))
            for d in range(rb):
                loy_out[:, lanes_of(type_lane(d))] = old_in[d] + clip * last_in[d]
        else:
            tbl[0] = tbl[0] + clip * gap_mine

    with scope("drain"):
        arrive(loy.at[1:], flag("loy", 0))
        arrive(info.at[1:], flag("info", 0))
        arrive(blk.at[1:], flag("blk", 0))
        arrive(tbl.at[1:], flag("tq", 0))
        arrive(tmass.at[1:], flag("tm", 0))
        arrive(old.at[1:], flag("old", 0))
        arrive(last.at[1:], flag("last", 0))
        for it in range(ITERS):
            arrive(sums.at[it, 1:], flag("sums", it, 0))
            arrive(totals.at[it, 1:], flag("totals", it, 0))
            arrive(squares_in.at[it], flag("sq", it, 0))
            if it < ITERS - 1:
                arrive(means.at[it, 1:], flag("means", it, 0))
                arrive(gap.at[it, 1:], flag("gap", it, 0))
    assert len(names) == FLAGS


def local(
    mkt, grp,
    mean_utility, market_share, product_traits, taste_draws, taste_scale, type_weight,
    market_size, product_firm, firm_order, loyalty, firm_share,
):
    n_m, J, K = product_traits.shape
    firms, R = firm_share.shape
    owned = loyalty.shape[0]
    rb = R // LANES
    groups = mkt * grp // rb
    rows = n_m * J
    tiles = rows // LANES
    qr = firms // groups
    depth = n_m * (2 * K + 3)

    f32, bf16 = jnp.float32, jnp.bfloat16
    dma = pltpu.SemaphoreType.DMA
    vmem = pltpu.VMEM
    spec = pl.BlockSpec(memory_space=pltpu.VMEM)
    dims = (mkt, grp, rb, groups, n_m, J, K, firms, owned, R)
    scratch = [
        pltpu.SMEM((n_m,), f32),
        pltpu.SMEM((K,), f32),
        vmem((n_m, R), f32),
        vmem((K, n_m, J), f32),
        vmem((n_m, J), jnp.int32),
        vmem((n_m, J), f32),
        vmem((n_m, J), f32),
        vmem((firms // LANES, LANES), jnp.int32),
        vmem((firms, LANES), f32),
        vmem((rb, n_m * (K + 1), LANES), f32),
        vmem((rb, (K + 2) * tiles, LANES), f32),
        vmem((rb, owned, LANES), f32),
        vmem((ITERS - 1, rb, tiles, LANES), f32),
        vmem((groups, qr, LANES), f32),
        vmem((qr, LANES), f32),
        vmem((groups, 1, LANES), f32),
        vmem((1, LANES), f32),
        vmem((n_m, R), f32),
        vmem((rb, depth, rows), bf16),
        vmem((2, depth, 2 * LANES), bf16),
        vmem((rb * rows, firms), bf16),
        vmem((rb * rows, LANES), f32),
        vmem((rb * rows, LANES), f32),
        vmem((firms, LANES), f32),
        vmem((firms, LANES), f32),
        vmem((1, firms), f32),
        vmem((firms, 2 * LANES), bf16),
        vmem((2 * LANES, rb // 2 * rows), bf16),
        vmem((2 * LANES, rb // 2 * rows), bf16),
        vmem((LANES, firms // 2), f32),
        vmem((LANES, firms // 2), f32),
        vmem((ITERS, rb, tiles, LANES), f32),
        vmem((ITERS, rb, tiles, LANES), f32),
        vmem((ITERS, groups, qr, LANES), f32),
        vmem((ITERS, groups, qr, LANES), f32),
        vmem((ITERS - 1, groups, qr, LANES), f32),
        vmem((ITERS, 1, LANES), f32),
        vmem((ITERS, mkt * grp - 1, 1, LANES), f32),
        vmem((rb, owned, LANES), f32),
        vmem((rb, owned, LANES), f32),
        vmem((rb, owned, LANES), f32),
        vmem((rb, owned, LANES), f32),
        dma((11,)),
        dma((rb,)),
        dma((rb,)),
        dma((FLAGS,)),
    ]
    return pl.pallas_call(
        functools.partial(kernel, dims),
        out_shape=(
            pltpu.VMEM((n_m, J), f32),
            pltpu.VMEM((owned, R), f32),
        ),
        in_specs=[pl.BlockSpec(memory_space=pl.ANY)] * 11,
        out_specs=(spec, spec),
        scratch_shapes=scratch,
        compiler_params=pltpu.CompilerParams(
            collective_id=0, has_side_effects=True, vmem_limit_bytes=60 * 1024 * 1024
        ),
    )(
        market_size, taste_scale, taste_draws.transpose(1, 0, 2).reshape(n_m * K, R), type_weight,
        product_traits.transpose(2, 0, 1), product_firm, mean_utility, market_share,
        loyalty, firm_order.reshape(firms // LANES, LANES), firm_share,
    )


def solution(mesh):
    both = ("mkt", "grp")
    placed = (
        P(both, None), P(both, None), P(both, None, None), P(both, None, None), P(),
        P(both, None), P(both), P(both, None), P(), P(both, None), P(),
    )
    return jax.shard_map(
        functools.partial(local, mesh.shape["mkt"], mesh.shape["grp"]),
        mesh=mesh,
        in_specs=placed,
        out_specs=(P(both, None), P(both, None)),
        check_vma=False,
    )
```

```python
import functools

import jax
import jax.numpy as jnp
from jax import lax
from jax.experimental import pallas as pl
from jax.experimental.pallas import tpu as pltpu
from jax.sharding import PartitionSpec as P

ITERS = 3
FLAGS = 12 + 6 * ITERS + 6 * (ITERS - 1)
LANES = 128
MESH = pl.DeviceIdType.MESH

clip_target = 0.5
norm_eps = 1e-06

scope = jax.named_scope


def columns(row):
    return jnp.broadcast_to(row, (LANES, LANES)).T


def split_hi_lo(x):
    hi = x.astype(jnp.bfloat16)
    lo = (x - hi.astype(jnp.float32)).astype(jnp.bfloat16)
    return hi, lo


def xor(x, d, size):
    out = x
    bit = 1
    while bit < size:
        out = out + ((d // bit) % 2) * (1 - 2 * ((x // bit) % 2)) * bit
        bit *= 2
    return out


def kernel(
    dims,
    size_h, scale_h, draws_h, weight_h, traits_h, firm_h, mean_h, share_own_h, loy_h, order_h, share_h,
    mean_out, loy_out,
    size_ref, scale_ref, weight_ref, traits_ref, firm_ref, mean_ref, share_own_ref, order_ref, share_v,
    blk, info, loy, means, tbl, tq, tmass, tm_own,
    mass_own, lmat, rmats, one_hot, util, near_gap, col, order_col, order_row, table_hl, weighted_e, weighted_o,
    acc_e, acc_o,
    sums, sums_in, totals, totals_in, gap, squares, squares_in, old, old_in, last, last_in,
    in_s, blk_s, info_s, sem,
):
    mkt, grp, rb, groups, n_m, J, K, firms, owned, R = dims
    n = mkt * grp
    rows = n_m * J
    tiles = rows // LANES
    pair = LANES // J
    qr = firms // groups
    half = groups // 2
    near = half * qr
    pairs = rb // 2
    a = lax.axis_index("mkt")
    b = lax.axis_index("grp")
    ao, ai = a // rb, a % rb
    q_me = ao * grp + b
    me = a * grp + b

    def type_lane(d):
        return xor(ai, d, rb)

    def type_device(d):
        return (ao * rb + xor(ai, d, rb), b)

    def market_device(j):
        q = xor(q_me, j, groups)
        return ((q // grp) * rb + ai, q % grp)

    def lanes_of(p):
        return pl.ds(pl.multiple_of(p * LANES, LANES), LANES)

    names = {}

    def flag(*key):
        return sem.at[names.setdefault(key, len(names))]

    def send(src, dst, out_sem, in_sem, device):
        pltpu.make_async_remote_copy(
            src_ref=src, dst_ref=dst, send_sem=out_sem, recv_sem=in_sem, device_id=device, device_id_type=MESH,
        ).start()

    def arrive(ref, in_sem):
        pltpu.make_async_copy(ref, ref, in_sem).wait()

    m0 = n_m * K

    def info_row(d, k, i):
        at = k * tiles + i
        return info[d, at:at + 1, :]

    def pack(x):
        return jnp.concatenate([x[i * tiles:(i + 1) * tiles, :] for i in range(pair)], axis=1)

    inputs = {}
    for at, (key, src, dst) in enumerate((
        ("weight", weight_h, weight_ref), ("traits", traits_h, traits_ref), ("firm", firm_h, firm_ref),
        ("mean", mean_h, mean_ref), ("size", size_h, size_ref), ("scale", scale_h, scale_ref),
        ("draws", draws_h.at[:, lanes_of(ai)], blk.at[0, :m0]), ("loy", loy_h.at[:, lanes_of(ai)], loy.at[0]),
        ("order", order_h, order_ref), ("share_own", share_own_h, share_own_ref),
        ("share", share_h.at[:, lanes_of(ai)], share_v),
    )):
        inputs[key] = pltpu.make_async_copy(src, dst, in_s.at[at])
        inputs[key].start()

    barrier = pltpu.get_barrier_semaphore()

    @pl.loop(1, n)
    def _(d):
        t = (me + d) % n
        pl.semaphore_signal(barrier, inc=1, device_id=(t // grp, t % grp), device_id_type=MESH)

    for key in ("weight", "traits", "firm", "mean", "size", "scale"):
        inputs[key].wait()
    for k in range(K):
        info[0, k * tiles:(k + 1) * tiles, :] = pack(traits_ref[k] * scale_ref[k])
    info[0, K * tiles:(K + 1) * tiles, :] = pack(firm_ref[...].astype(jnp.float32))
    mean_now = pack(mean_ref[...])
    info[0, (K + 1) * tiles:, :] = mean_now
    for m in range(n_m):
        mass_own[m:m + 1, :] = weight_ref[m:m + 1, :] * size_ref[m]

    with scope("bar"):
        pl.semaphore_wait(barrier, n - 1)

    for d in range(1, rb):
        send(loy_h.at[:, lanes_of(type_lane(d))], loy.at[d], flag("loy", 0), flag("loy", 1), type_device(d))
    for d in [1, *range(2, rb, 2)]:
        send(info.at[0], info.at[d], flag("info", 0), info_s.at[d], type_device(d))
    for d in range(1, rb):
        device = type_device(d)
        lanes = lanes_of(type_lane(d))
        send(draws_h.at[:, lanes], blk.at[d, :m0], flag("blk", 0), blk_s.at[d], device)
        send(mass_own.at[:, lanes], blk.at[d, m0:], flag("blk", 0), blk_s.at[d], device)

    def arrive_info(d):
        arrive(info.at[d], info_s.at[d])

    def hand_on(d):
        send(info.at[d], info.at[d + 1], flag("info", 0), info_s.at[d + 1], type_device(1))

    blk[0, m0:, :] = mass_own[:, lanes_of(ai)]
    weighted_o[:, (pairs - 1) * rows:] = jnp.zeros_like(weighted_o[:, (pairs - 1) * rows:])
    acc_e[...] = jnp.zeros_like(acc_e)
    acc_o[...] = jnp.zeros_like(acc_o)

    for key in ("order", "draws", "loy"):
        inputs[key].wait()
    for i in range(firms // LANES):
        col[i * LANES:(i + 1) * LANES, :] = columns(order_ref[i:i + 1, :].astype(jnp.float32))
    for j in range(groups):
        q = xor(q_me, j, groups)
        for d in range(rb):
            src = (((q // grp) * rb + xor(ai, d, rb)) * grp + q % grp) * owned
            dst = (j * rb + d) * owned
            order_col[dst:dst + owned, :] = col[pl.ds(pl.multiple_of(src, owned), owned), :]
    for i in range(firms // LANES):
        order_row[0:1, i * LANES:(i + 1) * LANES] = order_col[i * LANES:(i + 1) * LANES, :].T[0:1, :]

    kk = n_m * K
    row = lax.broadcasted_iota(jnp.int32, (n_m, LANES), 0)
    lane = lax.broadcasted_iota(jnp.int32, (n_m, LANES), 1)
    offset = row - (lane // J) * tiles
    zero = jnp.zeros((n_m, LANES), jnp.float32)
    rmats[:, kk:, :] = jnp.zeros_like(rmats[:, kk:, :])
    rmats[:, 2 * kk:, :LANES] = jnp.ones_like(rmats[:, 2 * kk:, :LANES])

    weighted = (weighted_e, weighted_o)

    def rows_of(d, r0, count):
        return pl.ds(pl.multiple_of(((d % 2) * pairs + d // 2) * rows + r0, LANES), count)

    def spread(part, where):
        return jnp.where(where, jnp.broadcast_to(part.astype(jnp.float32), (n_m, LANES)), zero).astype(jnp.bfloat16)

    def build(d):
        for i in range(tiles):
            here = offset == i
            at = slice(i * LANES, (i + 1) * LANES)
            for k in range(K):
                hi, lo = split_hi_lo(info_row(d, k, i))
                lmat[d, k * n_m:(k + 1) * n_m, at] = spread(hi, here)
                lmat[d, kk + k * n_m:kk + (k + 1) * n_m, at] = spread(lo, here)
            rest = info_row(d, K + 1, i)
            for s in range(3):
                hi = rest.astype(jnp.bfloat16)
                rest = rest - hi.astype(jnp.float32)
                lmat[d, 2 * kk + s * n_m:2 * kk + (s + 1) * n_m, at] = spread(hi, here)
        for i in range(tiles):
            firm_col = columns(info_row(d, K, i))
            for f in range(firms // LANES):
                one_hot[rows_of(d, i * LANES, LANES), f * LANES:(f + 1) * LANES] = (
                    firm_col == order_row[0:1, f * LANES:(f + 1) * LANES]
                ).astype(jnp.float32).astype(jnp.bfloat16)

    def taste(d, par):
        rmat = rmats.at[par]
        hi, lo = split_hi_lo(blk[d, :m0, :])
        rmat[:kk, :LANES] = hi
        rmat[:kk, LANES:] = lo
        rmat[kk:2 * kk, :LANES] = hi
        both = lax.dot_general(
            lmat[d], rmat[...], (((0,), (0,)), ((), ())), preferred_element_type=jnp.float32
        )
        util[rows_of(d, 0, rows), :] = both[:, :LANES] + both[:, LANES:]

    with scope("prep0"):
        build(0)
        taste(0, 0)
    with scope("share"):
        inputs["share"].wait()
        inputs["share_own"].wait()
        mine_col = order_col[:qr, :]
        number = lax.broadcasted_iota(jnp.int32, (qr, LANES), 1).astype(jnp.float32)
        my_share = jnp.zeros((qr, LANES), jnp.float32)
        for i in range(firms // LANES):
            pick = (mine_col == number + float(i * LANES)).astype(jnp.float32)
            my_share += jnp.dot(
                pick, share_v[i * LANES:(i + 1) * LANES, :],
                precision=lax.Precision.HIGHEST, preferred_element_type=jnp.float32,
            )
        my_share = jnp.log(my_share)
        base = jnp.log(share_own_ref[...]) + jnp.log(jnp.sum(mass_own[...], axis=1, keepdims=True))
        base = pack(base)

    with scope("arr_i2"):
        arrive_info(2)
    hand_on(2)
    with scope("arr_i1"):
        arrive_info(1)

    @pl.loop(1, 3)
    def _(d):
        with scope("build12"):
            build(d)

    with scope("arr_loy"):
        arrive(loy.at[1:], flag("loy", 1))
    for d in range(rb):
        tq[d * owned:(d + 1) * owned, :] = loy[d]
    for j in range(1, groups):
        send(tq, tbl.at[j], flag("tq", 0), flag("tq", 1), market_device(j))
    tbl[0] = tq[...]

    @pl.loop(2, pairs)
    def _(i):
        with scope("arr_ie"):
            arrive_info(2 * i)
        hand_on(2 * i)
        build(2 * i)

    def arrive_inputs(d):
        arrive(blk.at[d], blk_s.at[d])

    @pl.loop(1, 3)
    def _(d):
        with scope("arr_a"):
            arrive_inputs(d)
        with scope("prep_a"):
            taste(d, 0)

    @pl.loop(1, pairs)
    def _(i):
        with scope("arr_io"):
            arrive_info(2 * i + 1)
        build(2 * i + 1)

    first = rb // 2

    @pl.loop(3, first)
    def _(d):
        with scope("arr_a"):
            arrive_inputs(d)
        with scope("prep_a"):
            taste(d, 0)

    with scope("arr_tbl"):
        arrive(tbl.at[1:], flag("tq", 1))

    def split_into(j, value):
        hi, lo = split_hi_lo(value)
        table_hl[j * qr:(j + 1) * qr, :LANES] = hi
        table_hl[j * qr:(j + 1) * qr, LANES:] = lo

    for j in range(groups):
        split_into(j, tbl[j])

    per_block = 2
    block = per_block * LANES

    def gather(d, r0, begin, end):
        both = jnp.dot(
            one_hot[rows_of(d, r0, block), begin:end], table_hl[begin:end, :], preferred_element_type=jnp.float32
        )
        return both[:, :LANES] + both[:, LANES:]

    def shares(it, i, par, clip, other):
        d = 2 * i + par
        moved = None
        for h in range(rows // block):
            r0 = h * block
            at = rows_of(d, r0, block)
            if it == 0:
                u = util[at, :] + gather(d, r0, 0, firms)
            else:
                u = util[at, :] + clip * (near_gap[at, :] + gather(d, r0, near, firms))
            if it < ITERS - 1:
                util[at, :] = u
            chunk = far_part(other, 1 - par, r0, block)
            moved = chunk if moved is None else moved + chunk
            expu = jnp.exp(u)
            for c in range(per_block):
                t = h * per_block + c
                parts = []
                for s in range(pair):
                    part = expu[c * LANES + s * J:c * LANES + (s + 1) * J, :]
                    m = s * tiles + t
                    parts.append(
                        part * (blk[d, m0 + m:m0 + m + 1, :] / (1.0 + jnp.sum(part, axis=0, keepdims=True)))
                    )
                bought = jnp.concatenate(parts, axis=0).T
                sums[it, d, t:t + 1, :] = jnp.sum(bought, axis=0, keepdims=True)
                hi, lo = split_hi_lo(bought)
                lanes = pl.ds(pl.multiple_of(i * rows + t * LANES, LANES), LANES)
                weighted[par][:LANES, lanes] = hi
                weighted[par][LANES:, lanes] = lo
        return moved

    def far_part(i, par, r0, count):
        lanes = pl.ds(pl.multiple_of(i * rows + r0, LANES), count)
        part = jnp.dot(
            weighted[par][:, lanes], one_hot[rows_of(2 * i + par, r0, count), near:],
            preferred_element_type=jnp.float32,
        )
        return part[:LANES, :] + part[LANES:, :]

    def pair_step(it, s, clip, ready):
        i = s if it == 0 else pairs - 1 - s
        prev = (s + pairs - 1) % pairs if it == 0 else (pairs - s) % pairs
        started = s > 0
        ready(i)
        part = shares(it, i, 0, clip, prev)
        acc_o[...] = jnp.where(started, acc_o[...] + part, 0.0)
        part = shares(it, i, 1, clip, i)
        acc_e[...] = jnp.where(started, acc_e[...], 0.0) + part
        send_sums(it, 2 * i + 1)

        if isinstance(i, int):
            if i:
                send_sums(it, 2 * i)
        else:
            @pl.when(i > 0)
            def _():
                send_sums(it, 2 * i)

    def send_sums(it, d):
        send(sums.at[it, d], sums_in.at[it, d], flag("sums", it, 0), flag("sums", it, 1), type_device(d))

    def by_firm(x):
        return jnp.concatenate([x[:, i * LANES:(i + 1) * LANES].T for i in range(near // LANES)], axis=0)

    def far_totals(it):
        acc = by_firm(acc_e[...] + acc_o[...] + far_part(pairs - 1 if it == 0 else 0, 1, 0, rows))
        for j in range(half):
            totals[it, half + j] = acc[j * qr:(j + 1) * qr, :]

    def near_totals(it):
        acc = None
        for par in range(2):
            part = jnp.dot(
                weighted[par][...], one_hot[par * pairs * rows:(par + 1) * pairs * rows, :near],
                preferred_element_type=jnp.float32,
            )
            part = by_firm(part[:LANES, :] + part[LANES:, :])
            acc = part if acc is None else acc + part
        for j in range(half):
            totals[it, j] = acc[j * qr:(j + 1) * qr, :]

    clip = None
    log_mass = None
    for it in range(ITERS):
        final = it == ITERS - 1
        if it == 0:
            with scope("sh_a"):
                for i in range(first // 2):
                    pair_step(0, i, None, lambda d: None)

            def ready(i):
                with scope("arr_b"):
                    for par in range(2):
                        arrive_inputs(2 * i + par)
                with scope("taste_b"):
                    for par in range(2):
                        taste(2 * i + par, par)

            @pl.loop(first // 2, pairs)
            def _(i):
                pair_step(0, i, None, ready)

            tm_own[...] = jnp.zeros_like(tm_own)
            for d in range(rb):
                tm_own[...] += jnp.sum(blk[d, m0:, :], axis=0, keepdims=True)
            for j in range(1, groups):
                send(tm_own, tmass.at[j], flag("tm", 0), flag("tm", 1), market_device(j))
            tmass[0] = tm_own[...]
        else:
            with scope("shares%d" % it):
                for i in range(pairs):
                    pair_step(it, i, clip, lambda d: None)

        sums_in[it, 0] = sums[it, 0]

        with scope("far%d" % it):
            far_totals(it)
        for j in range(half, groups):
            send(totals.at[it, j], totals_in.at[it, j], flag("totals", it, 0), flag("totals", it, 1), market_device(j))
        with scope("near%d" % it):
            near_totals(it)
        for j in range(1, half):
            send(totals.at[it, j], totals_in.at[it, j], flag("totals", it, 0), flag("totals", it, 1), market_device(j))
        totals_in[it, 0] = totals[it, 0]

        if final:
            for d in range(rb):
                old[d] = tbl[0, d * owned:(d + 1) * owned, :]
            for d in range(1, rb):
                send(old.at[d], old_in.at[d], flag("old", 0), flag("old", 1), type_device(d))
            old_in[0] = old[0]

        if it == 0:
            arrive(tmass.at[1:], flag("tm", 1))
            log_mass = jnp.log(jnp.sum(tmass[...], axis=0))

        def settle_means(mean_now):
            with scope("arr_sums%d" % it):
                arrive(sums_in.at[it, 1:], flag("sums", it, 1))
            step = base - jnp.log(jnp.sum(sums_in[it], axis=0))
            mean_now = mean_now + step
            if final:
                for i in range(pair):
                    mean_out[i * tiles:(i + 1) * tiles, :] = mean_now[:, i * J:(i + 1) * J]
            else:
                means[it, 0] = step
                for d in range(1, rb):
                    send(means.at[it, 0], means.at[it, d], flag("means", it, 0), flag("means", it, 1), type_device(d))
            return mean_now

        if it:
            mean_now = settle_means(mean_now)
        with scope("arr_tot%d" % it):
            arrive(totals_in.at[it, 1:], flag("totals", it, 1))
        gap_mine = my_share - (jnp.log(jnp.sum(totals_in[it], axis=0)) - log_mass)
        squares[it] = jnp.sum(gap_mine * gap_mine, axis=0, keepdims=True)

        def send_squares():
            @pl.loop(1, n)
            def _(d):
                t = (me + d) % n
                send(
                    squares.at[it], squares_in.at[it, d - 1], flag("sq", it, 0), flag("sq", it, 1), (t // grp, t % grp)
                )

        if final:
            for d in range(rb):
                last[d] = gap_mine[d * owned:(d + 1) * owned, :]
            for d in range(1, rb):
                send(last.at[d], last_in.at[d], flag("last", 0), flag("last", 1), type_device(d))
            last_in[0] = last[0]
            send_squares()
        else:
            gap[it, 0] = gap_mine
            for j in [half, *range(1, half)]:
                send(gap.at[it, 0], gap.at[it, j], flag("gap", it, 0), flag("gap", it, 1 + j // half), market_device(j))
            send_squares()
            if it == 0:
                mean_now = settle_means(mean_now)
            def add_near():
                with scope("arr_gapn%d" % it):
                    split_into(0, gap_mine)
                    arrive(gap.at[it, 1:half], flag("gap", it, 1))
                    for j in range(1, half):
                        split_into(j, gap[it, j])

                with scope("gnear%d" % it):
                    @pl.loop(0, pairs // 2)
                    def _(i):
                        for par in range(4):
                            at = rows_of(4 * i + par, 0, rows)
                            both = jnp.dot(one_hot[at, :near], table_hl[:near, :], preferred_element_type=jnp.float32)
                            near_gap[at, :] = both[:, :LANES] + both[:, LANES:]

            def add_means():
                with scope("arr_mean%d" % it):
                    arrive(means.at[it, 1:], flag("means", it, 1))

                with scope("addmean%d" % it):
                    @pl.loop(0, pairs)
                    def _(i):
                        for par in range(2):
                            for t in range(tiles):
                                at = rows_of(2 * i + par, t * LANES, LANES)
                                util[at, :] = util[at, :] + columns(means[it, 2 * i + par, t:t + 1, :])

            def hand_gap():
                with scope("arr_gapy%d" % it):
                    arrive(gap.at[it, half], flag("gap", it, 2))
                for j in range(1, half):
                    send(
                        gap.at[it, half], gap.at[it, half + j], flag("gap", it, 0), flag("gap", it, 3), market_device(j)
                    )

            add_near()
            hand_gap()
            add_means()

            with scope("arr_gap%d" % it):
                arrive(gap.at[it, half + 1:], flag("gap", it, 3))
                for j in range(half, groups):
                    split_into(j, gap[it, j])

        with scope("arr_sq%d" % it):
            arrive(squares_in.at[it], flag("sq", it, 1))
        total = jnp.sum(jnp.sum(squares_in[it], axis=0) + squares[it], axis=1, keepdims=True)
        clip = jnp.minimum(1.0, clip_target / jnp.sqrt(total / (firms * R) + norm_eps))

        if final:
            with scope("arr_last"):
                arrive(old_in.at[1:], flag("old", 1))
                arrive(last_in.at[1:], flag("last", 1))
            for d in range(rb):
                loy_out[:, lanes_of(type_lane(d))] = old_in[d] + clip * last_in[d]
        else:
            tbl[0] = tbl[0] + clip * gap_mine

    with scope("drain"):
        arrive(loy.at[1:], flag("loy", 0))
        arrive(info.at[1:], flag("info", 0))
        arrive(blk.at[1:], flag("blk", 0))
        arrive(tbl.at[1:], flag("tq", 0))
        arrive(tmass.at[1:], flag("tm", 0))
        arrive(old.at[1:], flag("old", 0))
        arrive(last.at[1:], flag("last", 0))
        for it in range(ITERS):
            arrive(sums.at[it, 1:], flag("sums", it, 0))
            arrive(totals.at[it, 1:], flag("totals", it, 0))
            arrive(squares_in.at[it], flag("sq", it, 0))
            if it < ITERS - 1:
                arrive(means.at[it, 1:], flag("means", it, 0))
                arrive(gap.at[it, 1:], flag("gap", it, 0))
    assert len(names) == FLAGS


def local(
    mkt, grp,
    mean_utility, market_share, product_traits, taste_draws, taste_scale, type_weight,
    market_size, product_firm, firm_order, loyalty, firm_share,
):
    n_m, J, K = product_traits.shape
    firms, R = firm_share.shape
    owned = loyalty.shape[0]
    rb = R // LANES
    groups = mkt * grp // rb
    rows = n_m * J
    tiles = rows // LANES
    qr = firms // groups
    depth = n_m * (2 * K + 3)

    f32, bf16 = jnp.float32, jnp.bfloat16
    dma = pltpu.SemaphoreType.DMA
    vmem = pltpu.VMEM
    spec = pl.BlockSpec(memory_space=pltpu.VMEM)
    dims = (mkt, grp, rb, groups, n_m, J, K, firms, owned, R)
    scratch = [
        pltpu.SMEM((n_m,), f32),
        pltpu.SMEM((K,), f32),
        vmem((n_m, R), f32),
        vmem((K, n_m, J), f32),
        vmem((n_m, J), jnp.int32),
        vmem((n_m, J), f32),
        vmem((n_m, J), f32),
        vmem((firms // LANES, LANES), jnp.int32),
        vmem((firms, LANES), f32),
        vmem((rb, n_m * (K + 1), LANES), f32),
        vmem((rb, (K + 2) * tiles, LANES), f32),
        vmem((rb, owned, LANES), f32),
        vmem((ITERS - 1, rb, tiles, LANES), f32),
        vmem((groups, qr, LANES), f32),
        vmem((qr, LANES), f32),
        vmem((groups, 1, LANES), f32),
        vmem((1, LANES), f32),
        vmem((n_m, R), f32),
        vmem((rb, depth, rows), bf16),
        vmem((2, depth, 2 * LANES), bf16),
        vmem((rb * rows, firms), bf16),
        vmem((rb * rows, LANES), f32),
        vmem((rb * rows, LANES), f32),
        vmem((firms, LANES), f32),
        vmem((firms, LANES), f32),
        vmem((1, firms), f32),
        vmem((firms, 2 * LANES), bf16),
        vmem((2 * LANES, rb // 2 * rows), bf16),
        vmem((2 * LANES, rb // 2 * rows), bf16),
        vmem((LANES, firms // 2), f32),
        vmem((LANES, firms // 2), f32),
        vmem((ITERS, rb, tiles, LANES), f32),
        vmem((ITERS, rb, tiles, LANES), f32),
        vmem((ITERS, groups, qr, LANES), f32),
        vmem((ITERS, groups, qr, LANES), f32),
        vmem((ITERS - 1, groups, qr, LANES), f32),
        vmem((ITERS, 1, LANES), f32),
        vmem((ITERS, mkt * grp - 1, 1, LANES), f32),
        vmem((rb, owned, LANES), f32),
        vmem((rb, owned, LANES), f32),
        vmem((rb, owned, LANES), f32),
        vmem((rb, owned, LANES), f32),
        dma((11,)),
        dma((rb,)),
        dma((rb,)),
        dma((FLAGS,)),
    ]
    return pl.pallas_call(
        functools.partial(kernel, dims),
        out_shape=(
            pltpu.VMEM((n_m, J), f32),
            pltpu.VMEM((owned, R), f32),
        ),
        in_specs=[pl.BlockSpec(memory_space=pl.ANY)] * 11,
        out_specs=(spec, spec),
        scratch_shapes=scratch,
        compiler_params=pltpu.CompilerParams(
            collective_id=0, has_side_effects=True, vmem_limit_bytes=60 * 1024 * 1024
        ),
    )(
        market_size, taste_scale, taste_draws.transpose(1, 0, 2).reshape(n_m * K, R), type_weight,
        product_traits.transpose(2, 0, 1), product_firm, mean_utility, market_share,
        loyalty, firm_order.reshape(firms // LANES, LANES), firm_share,
    )


def solution(mesh):
    both = ("mkt", "grp")
    placed = (
        P(both, None), P(both, None), P(both, None, None), P(both, None, None), P(),
        P(both, None), P(both), P(both, None), P(), P(both, None), P(),
    )
    return jax.shard_map(
        functools.partial(local, mesh.shape["mkt"], mesh.shape["grp"]),
        mesh=mesh,
        in_specs=placed,
        out_specs=(P(both, None), P(both, None)),
        check_vma=False,
    )
```

```python
import functools

import jax
import jax.numpy as jnp
from jax import lax
from jax.experimental import pallas as pl
from jax.experimental.pallas import tpu as pltpu
from jax.sharding import PartitionSpec as P

ITERS = 3
FLAGS = 12 + 6 * ITERS + 6 * (ITERS - 1)
LANES = 128
MESH = pl.DeviceIdType.MESH

clip_target = 0.5
norm_eps = 1e-06

scope = jax.named_scope


def columns(row):
    return jnp.broadcast_to(row, (LANES, LANES)).T


def split_hi_lo(x):
    hi = x.astype(jnp.bfloat16)
    lo = (x - hi.astype(jnp.float32)).astype(jnp.bfloat16)
    return hi, lo


def xor(x, d, size):
    out = x
    bit = 1
    while bit < size:
        out = out + ((d // bit) % 2) * (1 - 2 * ((x // bit) % 2)) * bit
        bit *= 2
    return out


def kernel(
    dims,
    size_h, scale_h, draws_h, weight_h, traits_h, firm_h, mean_h, share_own_h, loy_h, order_h, share_h,
    mean_out, loy_out,
    size_ref, scale_ref, weight_ref, traits_ref, firm_ref, mean_ref, share_own_ref, order_ref, share_v,
    blk, info, loy, means, tbl, tq, tmass, tm_own,
    mass_own, lmat, rmats, one_hot, util, near_gap, col, order_col, order_row, table_hl, weighted_e, weighted_o,
    acc_e, acc_o,
    sums, sums_in, totals, totals_in, gap, squares, squares_in, old, old_in, last, last_in,
    in_s, blk_s, info_s, sem,
):
    mkt, grp, rb, groups, n_m, J, K, firms, owned, R = dims
    n = mkt * grp
    rows = n_m * J
    tiles = rows // LANES
    pair = LANES // J
    qr = firms // groups
    half = groups // 2
    near = half * qr
    pairs = rb // 2
    a = lax.axis_index("mkt")
    b = lax.axis_index("grp")
    ao, ai = a // rb, a % rb
    q_me = ao * grp + b
    me = a * grp + b

    def type_lane(d):
        return xor(ai, d, rb)

    def type_device(d):
        return (ao * rb + xor(ai, d, rb), b)

    def market_device(j):
        q = xor(q_me, j, groups)
        return ((q // grp) * rb + ai, q % grp)

    def lanes_of(p):
        return pl.ds(pl.multiple_of(p * LANES, LANES), LANES)

    names = {}

    def flag(*key):
        return sem.at[names.setdefault(key, len(names))]

    def send(src, dst, out_sem, in_sem, device):
        pltpu.make_async_remote_copy(
            src_ref=src, dst_ref=dst, send_sem=out_sem, recv_sem=in_sem, device_id=device, device_id_type=MESH,
        ).start()

    def arrive(ref, in_sem):
        pltpu.make_async_copy(ref, ref, in_sem).wait()

    m0 = n_m * K

    def info_row(d, k, i):
        at = k * tiles + i
        return info[d, at:at + 1, :]

    def pack(x):
        return jnp.concatenate([x[i * tiles:(i + 1) * tiles, :] for i in range(pair)], axis=1)

    inputs = {}
    for at, (key, src, dst) in enumerate((
        ("weight", weight_h, weight_ref), ("traits", traits_h, traits_ref), ("firm", firm_h, firm_ref),
        ("mean", mean_h, mean_ref), ("size", size_h, size_ref), ("scale", scale_h, scale_ref),
        ("draws", draws_h.at[:, lanes_of(ai)], blk.at[0, :m0]), ("loy", loy_h.at[:, lanes_of(ai)], loy.at[0]),
        ("order", order_h, order_ref), ("share_own", share_own_h, share_own_ref),
        ("share", share_h.at[:, lanes_of(ai)], share_v),
    )):
        inputs[key] = pltpu.make_async_copy(src, dst, in_s.at[at])
        inputs[key].start()

    barrier = pltpu.get_barrier_semaphore()

    for d in range(1, rb):
        pl.semaphore_signal(barrier, inc=1, device_id=type_device(d), device_id_type=MESH)
    for j in range(1, groups):
        pl.semaphore_signal(barrier, inc=1, device_id=market_device(j), device_id_type=MESH)

    for key in ("weight", "traits", "firm", "mean", "size", "scale"):
        inputs[key].wait()
    for k in range(K):
        info[0, k * tiles:(k + 1) * tiles, :] = pack(traits_ref[k] * scale_ref[k])
    info[0, K * tiles:(K + 1) * tiles, :] = pack(firm_ref[...].astype(jnp.float32))
    mean_now = pack(mean_ref[...])
    info[0, (K + 1) * tiles:, :] = mean_now
    for m in range(n_m):
        mass_own[m:m + 1, :] = weight_ref[m:m + 1, :] * size_ref[m]

    with scope("bar"):
        pl.semaphore_wait(barrier, rb + groups - 2)

    for d in range(1, rb):
        send(loy_h.at[:, lanes_of(type_lane(d))], loy.at[d], flag("loy", 0), flag("loy", 1), type_device(d))
    for d in [1, *range(2, rb, 2)]:
        send(info.at[0], info.at[d], flag("info", 0), info_s.at[d], type_device(d))
    for d in range(1, rb):
        device = type_device(d)
        lanes = lanes_of(type_lane(d))
        send(draws_h.at[:, lanes], blk.at[d, :m0], flag("blk", 0), blk_s.at[d], device)
        send(mass_own.at[:, lanes], blk.at[d, m0:], flag("blk", 0), blk_s.at[d], device)

    def arrive_info(d):
        arrive(info.at[d], info_s.at[d])

    def hand_on(d):
        send(info.at[d], info.at[d + 1], flag("info", 0), info_s.at[d + 1], type_device(1))

    blk[0, m0:, :] = mass_own[:, lanes_of(ai)]
    weighted_o[:, (pairs - 1) * rows:] = jnp.zeros_like(weighted_o[:, (pairs - 1) * rows:])
    acc_e[...] = jnp.zeros_like(acc_e)
    acc_o[...] = jnp.zeros_like(acc_o)

    for key in ("order", "draws", "loy"):
        inputs[key].wait()
    for i in range(firms // LANES):
        col[i * LANES:(i + 1) * LANES, :] = columns(order_ref[i:i + 1, :].astype(jnp.float32))
    for j in range(groups):
        q = xor(q_me, j, groups)
        for d in range(rb):
            src = (((q // grp) * rb + xor(ai, d, rb)) * grp + q % grp) * owned
            dst = (j * rb + d) * owned
            order_col[dst:dst + owned, :] = col[pl.ds(pl.multiple_of(src, owned), owned), :]
    for i in range(firms // LANES):
        order_row[0:1, i * LANES:(i + 1) * LANES] = order_col[i * LANES:(i + 1) * LANES, :].T[0:1, :]

    kk = n_m * K
    row = lax.broadcasted_iota(jnp.int32, (n_m, LANES), 0)
    lane = lax.broadcasted_iota(jnp.int32, (n_m, LANES), 1)
    offset = row - (lane // J) * tiles
    zero = jnp.zeros((n_m, LANES), jnp.float32)
    rmats[:, kk:, :] = jnp.zeros_like(rmats[:, kk:, :])
    rmats[:, 2 * kk:, :LANES] = jnp.ones_like(rmats[:, 2 * kk:, :LANES])

    weighted = (weighted_e, weighted_o)

    def rows_of(d, r0, count):
        return pl.ds(pl.multiple_of(((d % 2) * pairs + d // 2) * rows + r0, LANES), count)

    def spread(part, where):
        return jnp.where(where, jnp.broadcast_to(part.astype(jnp.float32), (n_m, LANES)), zero).astype(jnp.bfloat16)

    def build(d):
        for i in range(tiles):
            here = offset == i
            at = slice(i * LANES, (i + 1) * LANES)
            for k in range(K):
                hi, lo = split_hi_lo(info_row(d, k, i))
                lmat[d, k * n_m:(k + 1) * n_m, at] = spread(hi, here)
                lmat[d, kk + k * n_m:kk + (k + 1) * n_m, at] = spread(lo, here)
            rest = info_row(d, K + 1, i)
            for s in range(3):
                hi = rest.astype(jnp.bfloat16)
                rest = rest - hi.astype(jnp.float32)
                lmat[d, 2 * kk + s * n_m:2 * kk + (s + 1) * n_m, at] = spread(hi, here)
        for i in range(tiles):
            firm_col = columns(info_row(d, K, i))
            for f in range(firms // LANES):
                one_hot[rows_of(d, i * LANES, LANES), f * LANES:(f + 1) * LANES] = (
                    firm_col == order_row[0:1, f * LANES:(f + 1) * LANES]
                ).astype(jnp.float32).astype(jnp.bfloat16)

    def taste(d, par):
        rmat = rmats.at[par]
        hi, lo = split_hi_lo(blk[d, :m0, :])
        rmat[:kk, :LANES] = hi
        rmat[:kk, LANES:] = lo
        rmat[kk:2 * kk, :LANES] = hi
        both = lax.dot_general(
            lmat[d], rmat[...], (((0,), (0,)), ((), ())), preferred_element_type=jnp.float32
        )
        util[rows_of(d, 0, rows), :] = both[:, :LANES] + both[:, LANES:]

    with scope("prep0"):
        build(0)
        taste(0, 0)
    with scope("share"):
        inputs["share"].wait()
        inputs["share_own"].wait()
        mine_col = order_col[:qr, :]
        number = lax.broadcasted_iota(jnp.int32, (qr, LANES), 1).astype(jnp.float32)
        my_share = jnp.zeros((qr, LANES), jnp.float32)
        for i in range(firms // LANES):
            pick = (mine_col == number + float(i * LANES)).astype(jnp.float32)
            my_share += jnp.dot(
                pick, share_v[i * LANES:(i + 1) * LANES, :],
                precision=lax.Precision.HIGHEST, preferred_element_type=jnp.float32,
            )
        my_share = jnp.log(my_share)
        base = jnp.log(share_own_ref[...]) + jnp.log(jnp.sum(mass_own[...], axis=1, keepdims=True))
        base = pack(base)

    with scope("arr_i2"):
        arrive_info(2)
    hand_on(2)
    with scope("arr_i1"):
        arrive_info(1)

    @pl.loop(1, 3)
    def _(d):
        with scope("build12"):
            build(d)

    with scope("arr_loy"):
        arrive(loy.at[1:], flag("loy", 1))
    for d in range(rb):
        tq[d * owned:(d + 1) * owned, :] = loy[d]
    for j in range(1, groups):
        send(tq, tbl.at[j], flag("tq", 0), flag("tq", 1), market_device(j))
    tbl[0] = tq[...]

    @pl.loop(2, pairs)
    def _(i):
        with scope("arr_ie"):
            arrive_info(2 * i)
        hand_on(2 * i)
        build(2 * i)

    def arrive_inputs(d):
        arrive(blk.at[d], blk_s.at[d])

    @pl.loop(1, 3)
    def _(d):
        with scope("arr_a"):
            arrive_inputs(d)
        with scope("prep_a"):
            taste(d, 0)

    @pl.loop(1, pairs)
    def _(i):
        with scope("arr_io"):
            arrive_info(2 * i + 1)
        build(2 * i + 1)

    first = rb // 2

    @pl.loop(3, first)
    def _(d):
        with scope("arr_a"):
            arrive_inputs(d)
        with scope("prep_a"):
            taste(d, 0)

    with scope("arr_tbl"):
        arrive(tbl.at[1:], flag("tq", 1))

    def split_into(j, value):
        hi, lo = split_hi_lo(value)
        table_hl[j * qr:(j + 1) * qr, :LANES] = hi
        table_hl[j * qr:(j + 1) * qr, LANES:] = lo

    for j in range(groups):
        split_into(j, tbl[j])

    per_block = 2
    block = per_block * LANES

    def gather(d, r0, begin, end):
        both = jnp.dot(
            one_hot[rows_of(d, r0, block), begin:end], table_hl[begin:end, :], preferred_element_type=jnp.float32
        )
        return both[:, :LANES] + both[:, LANES:]

    def shares(it, i, par, clip, other):
        d = 2 * i + par
        moved = None
        for h in range(rows // block):
            r0 = h * block
            at = rows_of(d, r0, block)
            if it == 0:
                u = util[at, :] + gather(d, r0, 0, firms)
            else:
                u = util[at, :] + clip * (near_gap[at, :] + gather(d, r0, near, firms))
            if it < ITERS - 1:
                util[at, :] = u
            chunk = far_part(other, 1 - par, r0, block)
            moved = chunk if moved is None else moved + chunk
            expu = jnp.exp(u)
            for c in range(per_block):
                t = h * per_block + c
                parts = []
                for s in range(pair):
                    part = expu[c * LANES + s * J:c * LANES + (s + 1) * J, :]
                    m = s * tiles + t
                    parts.append(
                        part * (blk[d, m0 + m:m0 + m + 1, :] / (1.0 + jnp.sum(part, axis=0, keepdims=True)))
                    )
                bought = jnp.concatenate(parts, axis=0).T
                sums[it, d, t:t + 1, :] = jnp.sum(bought, axis=0, keepdims=True)
                hi, lo = split_hi_lo(bought)
                lanes = pl.ds(pl.multiple_of(i * rows + t * LANES, LANES), LANES)
                weighted[par][:LANES, lanes] = hi
                weighted[par][LANES:, lanes] = lo
        return moved

    def far_part(i, par, r0, count):
        lanes = pl.ds(pl.multiple_of(i * rows + r0, LANES), count)
        part = jnp.dot(
            weighted[par][:, lanes], one_hot[rows_of(2 * i + par, r0, count), near:],
            preferred_element_type=jnp.float32,
        )
        return part[:LANES, :] + part[LANES:, :]

    def pair_step(it, s, clip, ready):
        i = s if it == 0 else pairs - 1 - s
        prev = (s + pairs - 1) % pairs if it == 0 else (pairs - s) % pairs
        started = s > 0
        ready(i)
        part = shares(it, i, 0, clip, prev)
        acc_o[...] = jnp.where(started, acc_o[...] + part, 0.0)
        part = shares(it, i, 1, clip, i)
        acc_e[...] = jnp.where(started, acc_e[...], 0.0) + part
        send_sums(it, 2 * i + 1)

        if isinstance(i, int):
            if i:
                send_sums(it, 2 * i)
        else:
            @pl.when(i > 0)
            def _():
                send_sums(it, 2 * i)

    def send_sums(it, d):
        send(sums.at[it, d], sums_in.at[it, d], flag("sums", it, 0), flag("sums", it, 1), type_device(d))

    def by_firm(x):
        return jnp.concatenate([x[:, i * LANES:(i + 1) * LANES].T for i in range(near // LANES)], axis=0)

    def far_totals(it):
        acc = by_firm(acc_e[...] + acc_o[...] + far_part(pairs - 1 if it == 0 else 0, 1, 0, rows))
        for j in range(half):
            totals[it, half + j] = acc[j * qr:(j + 1) * qr, :]

    def near_totals(it):
        acc = None
        for par in range(2):
            part = jnp.dot(
                weighted[par][...], one_hot[par * pairs * rows:(par + 1) * pairs * rows, :near],
                preferred_element_type=jnp.float32,
            )
            part = by_firm(part[:LANES, :] + part[LANES:, :])
            acc = part if acc is None else acc + part
        for j in range(half):
            totals[it, j] = acc[j * qr:(j + 1) * qr, :]

    clip = None
    log_mass = None
    for it in range(ITERS):
        final = it == ITERS - 1
        if it == 0:
            with scope("sh_a"):
                for i in range(first // 2):
                    pair_step(0, i, None, lambda d: None)

            def ready(i):
                with scope("arr_b"):
                    for par in range(2):
                        arrive_inputs(2 * i + par)
                with scope("taste_b"):
                    for par in range(2):
                        taste(2 * i + par, par)

            @pl.loop(first // 2, pairs)
            def _(i):
                pair_step(0, i, None, ready)

            tm_own[...] = jnp.zeros_like(tm_own)
            for d in range(rb):
                tm_own[...] += jnp.sum(blk[d, m0:, :], axis=0, keepdims=True)
            for j in range(1, groups):
                send(tm_own, tmass.at[j], flag("tm", 0), flag("tm", 1), market_device(j))
            tmass[0] = tm_own[...]
        else:
            with scope("shares%d" % it):
                for i in range(pairs):
                    pair_step(it, i, clip, lambda d: None)

        sums_in[it, 0] = sums[it, 0]

        with scope("far%d" % it):
            far_totals(it)
        for j in range(half, groups):
            send(totals.at[it, j], totals_in.at[it, j], flag("totals", it, 0), flag("totals", it, 1), market_device(j))
        with scope("near%d" % it):
            near_totals(it)
        for j in range(1, half):
            send(totals.at[it, j], totals_in.at[it, j], flag("totals", it, 0), flag("totals", it, 1), market_device(j))
        totals_in[it, 0] = totals[it, 0]

        if final:
            for d in range(rb):
                old[d] = tbl[0, d * owned:(d + 1) * owned, :]
            for d in range(1, rb):
                send(old.at[d], old_in.at[d], flag("old", 0), flag("old", 1), type_device(d))
            old_in[0] = old[0]

        if it == 0:
            arrive(tmass.at[1:], flag("tm", 1))
            log_mass = jnp.log(jnp.sum(tmass[...], axis=0))

        def settle_means(mean_now):
            with scope("arr_sums%d" % it):
                arrive(sums_in.at[it, 1:], flag("sums", it, 1))
            step = base - jnp.log(jnp.sum(sums_in[it], axis=0))
            mean_now = mean_now + step
            if final:
                for i in range(pair):
                    mean_out[i * tiles:(i + 1) * tiles, :] = mean_now[:, i * J:(i + 1) * J]
            else:
                means[it, 0] = step
                for d in range(1, rb):
                    send(means.at[it, 0], means.at[it, d], flag("means", it, 0), flag("means", it, 1), type_device(d))
            return mean_now

        if it:
            mean_now = settle_means(mean_now)
        with scope("arr_tot%d" % it):
            arrive(totals_in.at[it, 1:], flag("totals", it, 1))
        gap_mine = my_share - (jnp.log(jnp.sum(totals_in[it], axis=0)) - log_mass)
        squares[it] = jnp.sum(gap_mine * gap_mine, axis=0, keepdims=True)

        def send_squares():
            @pl.loop(1, n)
            def _(d):
                t = (me + d) % n
                send(
                    squares.at[it], squares_in.at[it, d - 1], flag("sq", it, 0), flag("sq", it, 1), (t // grp, t % grp)
                )

        if final:
            for d in range(rb):
                last[d] = gap_mine[d * owned:(d + 1) * owned, :]
            for d in range(1, rb):
                send(last.at[d], last_in.at[d], flag("last", 0), flag("last", 1), type_device(d))
            last_in[0] = last[0]
            send_squares()
        else:
            gap[it, 0] = gap_mine
            for j in [half, *range(1, half)]:
                send(gap.at[it, 0], gap.at[it, j], flag("gap", it, 0), flag("gap", it, 1 + j // half), market_device(j))
            send_squares()
            if it == 0:
                mean_now = settle_means(mean_now)
            def add_near():
                with scope("arr_gapn%d" % it):
                    split_into(0, gap_mine)
                    arrive(gap.at[it, 1:half], flag("gap", it, 1))
                    for j in range(1, half):
                        split_into(j, gap[it, j])

                with scope("gnear%d" % it):
                    @pl.loop(0, pairs // 2)
                    def _(i):
                        for par in range(4):
                            at = rows_of(4 * i + par, 0, rows)
                            both = jnp.dot(one_hot[at, :near], table_hl[:near, :], preferred_element_type=jnp.float32)
                            near_gap[at, :] = both[:, :LANES] + both[:, LANES:]

            def add_means():
                with scope("arr_mean%d" % it):
                    arrive(means.at[it, 1:], flag("means", it, 1))

                with scope("addmean%d" % it):
                    @pl.loop(0, pairs)
                    def _(i):
                        for par in range(2):
                            for t in range(tiles):
                                at = rows_of(2 * i + par, t * LANES, LANES)
                                util[at, :] = util[at, :] + columns(means[it, 2 * i + par, t:t + 1, :])

            def hand_gap():
                with scope("arr_gapy%d" % it):
                    arrive(gap.at[it, half], flag("gap", it, 2))
                for j in range(1, half):
                    send(
                        gap.at[it, half], gap.at[it, half + j], flag("gap", it, 0), flag("gap", it, 3), market_device(j)
                    )

            add_near()
            hand_gap()
            add_means()

            with scope("arr_gap%d" % it):
                arrive(gap.at[it, half + 1:], flag("gap", it, 3))
                for j in range(half, groups):
                    split_into(j, gap[it, j])

        with scope("arr_sq%d" % it):
            arrive(squares_in.at[it], flag("sq", it, 1))
        total = jnp.sum(jnp.sum(squares_in[it], axis=0) + squares[it], axis=1, keepdims=True)
        clip = jnp.minimum(1.0, clip_target / jnp.sqrt(total / (firms * R) + norm_eps))

        if final:
            with scope("arr_last"):
                arrive(old_in.at[1:], flag("old", 1))
                arrive(last_in.at[1:], flag("last", 1))
            for d in range(rb):
                loy_out[:, lanes_of(type_lane(d))] = old_in[d] + clip * last_in[d]
        else:
            tbl[0] = tbl[0] + clip * gap_mine

    with scope("drain"):
        arrive(loy.at[1:], flag("loy", 0))
        arrive(info.at[1:], flag("info", 0))
        arrive(blk.at[1:], flag("blk", 0))
        arrive(tbl.at[1:], flag("tq", 0))
        arrive(tmass.at[1:], flag("tm", 0))
        arrive(old.at[1:], flag("old", 0))
        arrive(last.at[1:], flag("last", 0))
        for it in range(ITERS):
            arrive(sums.at[it, 1:], flag("sums", it, 0))
            arrive(totals.at[it, 1:], flag("totals", it, 0))
            arrive(squares_in.at[it], flag("sq", it, 0))
            if it < ITERS - 1:
                arrive(means.at[it, 1:], flag("means", it, 0))
                arrive(gap.at[it, 1:], flag("gap", it, 0))
    assert len(names) == FLAGS


def local(
    mkt, grp,
    mean_utility, market_share, product_traits, taste_draws, taste_scale, type_weight,
    market_size, product_firm, firm_order, loyalty, firm_share,
):
    n_m, J, K = product_traits.shape
    firms, R = firm_share.shape
    owned = loyalty.shape[0]
    rb = R // LANES
    groups = mkt * grp // rb
    rows = n_m * J
    tiles = rows // LANES
    qr = firms // groups
    depth = n_m * (2 * K + 3)

    f32, bf16 = jnp.float32, jnp.bfloat16
    dma = pltpu.SemaphoreType.DMA
    vmem = pltpu.VMEM
    spec = pl.BlockSpec(memory_space=pltpu.VMEM)
    dims = (mkt, grp, rb, groups, n_m, J, K, firms, owned, R)
    scratch = [
        pltpu.SMEM((n_m,), f32),
        pltpu.SMEM((K,), f32),
        vmem((n_m, R), f32),
        vmem((K, n_m, J), f32),
        vmem((n_m, J), jnp.int32),
        vmem((n_m, J), f32),
        vmem((n_m, J), f32),
        vmem((firms // LANES, LANES), jnp.int32),
        vmem((firms, LANES), f32),
        vmem((rb, n_m * (K + 1), LANES), f32),
        vmem((rb, (K + 2) * tiles, LANES), f32),
        vmem((rb, owned, LANES), f32),
        vmem((ITERS - 1, rb, tiles, LANES), f32),
        vmem((groups, qr, LANES), f32),
        vmem((qr, LANES), f32),
        vmem((groups, 1, LANES), f32),
        vmem((1, LANES), f32),
        vmem((n_m, R), f32),
        vmem((rb, depth, rows), bf16),
        vmem((2, depth, 2 * LANES), bf16),
        vmem((rb * rows, firms), bf16),
        vmem((rb * rows, LANES), f32),
        vmem((rb * rows, LANES), f32),
        vmem((firms, LANES), f32),
        vmem((firms, LANES), f32),
        vmem((1, firms), f32),
        vmem((firms, 2 * LANES), bf16),
        vmem((2 * LANES, rb // 2 * rows), bf16),
        vmem((2 * LANES, rb // 2 * rows), bf16),
        vmem((LANES, firms // 2), f32),
        vmem((LANES, firms // 2), f32),
        vmem((ITERS, rb, tiles, LANES), f32),
        vmem((ITERS, rb, tiles, LANES), f32),
        vmem((ITERS, groups, qr, LANES), f32),
        vmem((ITERS, groups, qr, LANES), f32),
        vmem((ITERS - 1, groups, qr, LANES), f32),
        vmem((ITERS, 1, LANES), f32),
        vmem((ITERS, mkt * grp - 1, 1, LANES), f32),
        vmem((rb, owned, LANES), f32),
        vmem((rb, owned, LANES), f32),
        vmem((rb, owned, LANES), f32),
        vmem((rb, owned, LANES), f32),
        dma((11,)),
        dma((rb,)),
        dma((rb,)),
        dma((FLAGS,)),
    ]
    return pl.pallas_call(
        functools.partial(kernel, dims),
        out_shape=(
            pltpu.VMEM((n_m, J), f32),
            pltpu.VMEM((owned, R), f32),
        ),
        in_specs=[pl.BlockSpec(memory_space=pl.ANY)] * 11,
        out_specs=(spec, spec),
        scratch_shapes=scratch,
        compiler_params=pltpu.CompilerParams(
            collective_id=0, has_side_effects=True, vmem_limit_bytes=60 * 1024 * 1024
        ),
    )(
        market_size, taste_scale, taste_draws.transpose(1, 0, 2).reshape(n_m * K, R), type_weight,
        product_traits.transpose(2, 0, 1), product_firm, mean_utility, market_share,
        loyalty, firm_order.reshape(firms // LANES, LANES), firm_share,
    )


def solution(mesh):
    both = ("mkt", "grp")
    placed = (
        P(both, None), P(both, None), P(both, None, None), P(both, None, None), P(),
        P(both, None), P(both), P(both, None), P(), P(both, None), P(),
    )
    return jax.shard_map(
        functools.partial(local, mesh.shape["mkt"], mesh.shape["grp"]),
        mesh=mesh,
        in_specs=placed,
        out_specs=(P(both, None), P(both, None)),
        check_vma=False,
    )
```
